32 devices in a mesh: view: 4 (over x, core), depth: 8 (over z, y).
Axes of the slice: x: 2, y: 2, z: 4, core: 2. Of those that a mesh axis runs over, the one named last changes fastest.
Arguments:
- volume: float32 [128, 128, 512], P(('view', 'depth')), may hold values from -6 to 6
- step_weights: float32 [4, 8, 64], P('view'), may hold values from -0.75 to 0.75
- row_interp: float32 [4, 64, 64], P('view'), may hold values from -0.75 to 0.75
- col_interp: float32 [4, 64, 64], P('view'), may hold values from -0.75 to 0.75
- tf_table: float32 [8, 8], replicated, may hold values from -3 to 3
- materials: int32 [2, 2, 8], P(None, None, 'depth'), may hold values from 0 to 7
- entry: int32 [4, 128, 128], P('view'), may hold values from 0 to 3
Outputs:
- picture: float32 [4, 3, 128, 128], P('view', None, 'depth')
The draws below stay inside these ranges and needn't reach their ends.
All inputs are finite; a program needn't handle non-finite values.
Results may differ from the reference program's by a relative error of at most 0.00018.
Values sent between devices are 32-bit elements; how exact they have to be, the bound alone decides.
No kernel may reach another device: no remote copies, remote signals or barrier semaphores. Data moves between devices by JAX's collectives and lax.ppermute only.
A program may use at most 64 MiB of HBM per device.

```python
import jax
import jax.numpy as jnp
from jax import lax

BRICK = 64
STEPS_B = 8
MATS = 8
NY = 128
NZ = 128
NX = 512
N_VIEW = 4
N_DEPTH = 8


def plant(result, stream_key, least, top_value):
    longest = result.shape.index(max(result.shape))
    spots = []
    for shift in (0, 1):
        where = [jax.random.randint(jax.random.fold_in(stream_key, axis), (), 0, length) for axis, length in enumerate(result.shape)]
        where[longest] = (where[longest] + shift) % result.shape[longest]
        spots.append(tuple(where))
    return result.at[spots[0]].set(least).at[spots[1]].set(top_value)


def steps_of(rng, dims, shards, low, largest):
    gain, own = 1.0, jax.random.fold_in(rng, 6)
    for axis_at, blocks in shards:
        heights = jnp.exp(jax.random.uniform(jax.random.fold_in(own, axis_at), (blocks,), jnp.float32, low / len(shards), largest / len(shards)))
        gain = gain * jnp.repeat(heights, dims[axis_at] // blocks).reshape([-1 if axis == axis_at else 1 for axis in range(len(dims))])
    return gain


def bell_draw(own_key, dims, scale, most, shards=(), kind=jnp.bfloat16):
    entries = scale * jax.random.normal(own_key, dims, jnp.float32)
    if shards:
        entries = entries * steps_of(own_key, dims, shards, -0.22, 0.18)
    return jnp.clip(entries, -most, most).astype(kind)


def setup_inputs(seed: int = 0) -> dict:
    arg_keys = jax.random.split(jax.random.key(seed), 8)
    volume = bell_draw(arg_keys[0], (NZ, NY, NX), 1.0, 6.0, ((0, 32),), jnp.float32)
    step_weights = bell_draw(arg_keys[1], (N_VIEW, STEPS_B, BRICK), BRICK ** -0.5, 0.75, ((0, 4),), jnp.float32)
    row_interp = bell_draw(arg_keys[2], (N_VIEW, BRICK, BRICK), BRICK ** -0.5, 0.75, ((0, 4),), jnp.float32)
    col_interp = bell_draw(arg_keys[3], (N_VIEW, BRICK, BRICK), BRICK ** -0.5, 0.75, ((0, 4),), jnp.float32)
    tf_table = bell_draw(arg_keys[4], (MATS, 8), 1.0, 3.0, (), jnp.float32)
    materials = plant(jax.random.randint(arg_keys[5], (NZ // BRICK, NY // BRICK, N_DEPTH), 0, MATS), jax.random.fold_in(arg_keys[5], 1), 0, MATS - 1).astype(jnp.int32)
    entry = plant(jax.random.randint(arg_keys[6], (N_VIEW, NZ, NY), 0, N_DEPTH // 2), jax.random.fold_in(arg_keys[6], 1), 0, (N_DEPTH // 2) - 1).astype(jnp.int32)
    return {"volume": volume, "step_weights": step_weights, "row_interp": row_interp, "col_interp": col_interp, "tf_table": tf_table, "materials": materials, "entry": entry}


def sample_brick(cells, steps_map, rows_map, cols_map):
    highest = lax.Precision.HIGHEST
    edge = rows_map.shape[0]
    first = jnp.einsum('zyi,si->szy', cells, steps_map, precision=highest)
    count_steps, total_rows, total_cols = first.shape
    second = first.reshape(count_steps, total_rows // edge, edge, total_cols)
    second = jnp.einsum('stky,rk->stry', second, rows_map, precision=highest)
    third = second.reshape(count_steps, total_rows, total_cols // edge, edge)
    third = jnp.einsum('szuj,cj->szuc', third, cols_map, precision=highest)
    return third.reshape(count_steps, total_rows, total_cols)


def expand_classes(classes, tf_table, edge):
    choices_range = jnp.arange(tf_table.shape[0], dtype=jnp.int32)
    onehot = (classes[:, :, None] == choices_range).astype(jnp.float32)
    tiles = jnp.einsum('abm,mc->cab', onehot, tf_table, precision=lax.Precision.HIGHEST)
    count_coef, tiles_rows, tiles_cols = tiles.shape
    spread = jnp.broadcast_to(tiles[:, :, None, :, None], (count_coef, tiles_rows, edge, tiles_cols, edge))
    return spread.reshape(count_coef, tiles_rows * edge, tiles_cols * edge)


def shade(samples, coefficients, live_mask, step_length):
    emission = jax.nn.softplus(coefficients[0:3, None] * samples[None] + coefficients[3:6, None])
    tau = step_length * live_mask[None] * jax.nn.softplus(coefficients[6][None] * samples + coefficients[7][None])
    earlier = jnp.cumsum(tau, axis=0) - tau
    weights = jnp.exp(-earlier) * (1.0 - jnp.exp(-tau))
    colours = jnp.sum(weights[None] * emission, axis=1)
    passed = jnp.exp(-jnp.sum(tau, axis=0))
    return colours, passed


def reference(volume, step_weights, row_interp, col_interp, tf_table, materials, entry):
    step_length = 2.0 / (STEPS_B * N_DEPTH)
    pictures = []
    for view_index in range(N_VIEW):
        picture = jnp.zeros((3, NZ, NY), jnp.float32)
        carried = jnp.ones((NZ, NY), jnp.float32)
        for depth_index in range(N_DEPTH):
            cells = volume[:, :, depth_index * BRICK:(depth_index + 1) * BRICK]
            samples = sample_brick(cells, step_weights[view_index], row_interp[view_index], col_interp[view_index])
            coefficients = expand_classes(materials[:, :, depth_index], tf_table, BRICK)
            live_mask = (entry[view_index] <= depth_index).astype(jnp.float32)
            colours, passed = shade(samples, coefficients, live_mask, step_length)
            picture = picture + carried[None] * colours
            carried = carried * passed
        pictures.append(picture)
    return jnp.stack(pictures)
```

```python
import functools

import jax
import jax.numpy as jnp
from jax import lax
from jax.experimental import pallas as pl
from jax.experimental.pallas import tpu as pltpu
from jax.sharding import PartitionSpec as P

LANES = 128
SUB = 8
COEF = 8
HIGHEST = lax.Precision.HIGHEST
NT = (((1,), (1,)), ((), ()))
NN = (((1,), (0,)), ((), ()))


def split(x):
    hi = x.astype(jnp.bfloat16)
    return hi, (x - hi.astype(jnp.float32)).astype(jnp.bfloat16)


def dot3(a, b, dims):
    dot = functools.partial(
        lax.dot_general, dimension_numbers=dims, preferred_element_type=jnp.float32
    )
    return dot(a[0], b[0]) + (dot(a[0], b[1]) + dot(a[1], b[0]))


def softplus(v):
    e = jnp.exp(-jnp.abs(v))
    small = e * (1.0 - 0.5 * e)
    return jnp.maximum(v, 0.0) + jnp.where(e < 1e-4, small, jnp.log(1.0 + e))


def send_kernel(depth, vol_ref, steps_ref, cols_ref, classes_ref, table_ref, out_ref):
    planes, lateral, span = vol_ref.shape
    views, steps, edge = steps_ref.shape
    bricks = span // edge
    tiles_z, tiles_y = classes_ref.shape[:2]
    per = lateral // depth

    weights = steps_ref[...].reshape(views * steps, edge)
    tiled = jnp.concatenate([weights] * bricks, axis=1)
    lane = lax.broadcasted_iota(jnp.int32, (bricks, span), 1)
    brick = lax.broadcasted_iota(jnp.int32, (bricks, span), 0)
    own = lane // edge == brick
    ray = jnp.where(own[None], tiled[:, None, :], 0.0).reshape(views * steps * bricks, span)
    cells = vol_ref[...].reshape(planes * lateral, span)
    first = dot3(split(cells), split(ray), NT)
    first_hi, first_lo = split(first)

    half = lax.broadcasted_iota(jnp.int32, (SUB, LANES), 1) < LANES // 2
    zero = jnp.zeros((edge, edge), jnp.float32)
    for pair in range(views // 2):
        rows = []
        for view in (2 * pair, 2 * pair + 1):
            c = cols_ref[view]
            for tile in range(tiles_y):
                rows.append(jnp.concatenate([c if t == tile else zero for t in range(tiles_y)], axis=1))
        maps = split(jnp.concatenate(rows, axis=0))
        for plane in range(planes):
            at = slice(plane * lateral, (plane + 1) * lateral)
            to = slice(pair * LANES, (pair + 1) * LANES)
            second = dot3(maps, (first_hi[at, to], first_lo[at, to]), NN)
            for k in range(2):
                for d in range(depth):
                    base = k * lateral + d * per
                    a = second[base : base + SUB]
                    b = second[base + SUB : base + 2 * SUB]
                    if k == 0:
                        b = pltpu.roll(b, LANES // 2, 1)
                    else:
                        a = pltpu.roll(a, LANES // 2, 1)
                    block = jnp.where(half, a, b)
                    out_ref[(2 * pair + k) * depth + d, plane * SUB : (plane + 1) * SUB, 0, :] = block

    lane = lax.broadcasted_iota(jnp.int32, (1, LANES), 1)
    for u in range(tiles_y):
        row = jnp.zeros((1, LANES), jnp.float32)
        for t in range(tiles_z):
            for ch in range(COEF):
                row = jnp.where(lane == t * COEF + ch, table_ref[classes_ref[t, u, 0], ch], row)
        for v in range(views):
            for d in range(depth):
                if d * per // edge == u:
                    out_ref[v * depth + d, planes * SUB : planes * SUB + 1, 0, :] = row


def render_kernel(step_length, recv_ref, maps_ref, entry_ref, out_ref, cells):
    sources, rows_block = recv_ref.shape[:2]
    data = rows_block - 1
    columns, rows = entry_ref.shape
    bricks = steps = SUB
    for s in range(sources):
        cells[s * data : (s + 1) * data, :] = recv_ref[s, 0:data, 0, :]
    maps = split(maps_ref[...])

    packed = jnp.concatenate([recv_ref[b, data : data + 1, 0, :] for b in range(bricks)], axis=0)
    lane = lax.broadcasted_iota(jnp.int32, (bricks, rows), 1)
    upper = lane >= rows // 2
    coef = []
    for ch in range(COEF):
        low = jnp.broadcast_to(packed[:, ch : ch + 1], (bricks, rows))
        high = jnp.broadcast_to(packed[:, COEF + ch : COEF + ch + 1], (bricks, rows))
        coef.append(jnp.where(upper, high, low))
    brick = lax.broadcasted_iota(jnp.int32, (bricks, rows), 0)

    shown = [[None] * columns for _ in range(3)]
    for x in range(SUB):
        planes = cells[pl.ds(x, rows, stride=SUB), :]
        samples = dot3(split(planes.T), maps, NN)
        for low in range(2):
            c = low * SUB + x
            live = jnp.where(entry_ref[c : c + 1, :] <= brick, step_length, 0.0)
            total = jnp.zeros((bricks, rows), jnp.float32)
            before = jnp.ones((bricks, rows), jnp.float32)
            colours = [jnp.zeros((bricks, rows), jnp.float32) for _ in range(3)]
            for s in range(steps):
                at = (low * steps + s) * bricks
                v = samples[at : at + bricks]
                total = total + live * softplus(coef[6] * v + coef[7])
                after = jnp.exp(-total)
                weight = before - after
                before = after
                for ch in range(3):
                    colours[ch] = colours[ch] + weight * softplus(coef[ch] * v + coef[3 + ch])
            front = total
            for shift in (1, 2, 4):
                front = front + jnp.where(brick >= shift, pltpu.roll(front, shift, 0), 0.0)
            reach = jnp.exp(total - front)
            for ch in range(3):
                shown[ch][c] = jnp.sum(reach * colours[ch], axis=0, keepdims=True)
    blank = jnp.zeros((LANES - 3 * columns, rows), jnp.float32)
    image = jnp.concatenate([r for ch in shown for r in ch] + [blank], axis=0)
    out_ref[...] = image.T.reshape(out_ref.shape)


def unpack_kernel(columns, recv_ref, out_ref):
    sources, rows, _ = recv_ref.shape
    owner = lax.broadcasted_iota(jnp.int32, (rows, LANES), 1) // columns
    for ch in range(3):
        out = jnp.zeros((rows, LANES), jnp.float32)
        for s in range(sources):
            moved = pltpu.roll(recv_ref[s], ((s - ch) * columns) % LANES, 1)
            out = jnp.where(owner == s, moved, out)
        out_ref[0, ch] = out


def vmem():
    return pl.BlockSpec(memory_space=pltpu.VMEM)


def smem():
    return pl.BlockSpec(memory_space=pltpu.SMEM)


def with_kernels(volume, all_steps, all_cols, row_interp, tf_table, materials, entry):
    views, steps, edge = all_steps.shape
    depth = lax.axis_size("depth")
    planes, lateral, span = volume.shape
    devices = views * depth
    per = lateral // depth
    rows = devices * planes
    step_length = 2.0 / (steps * depth)
    blocks = pl.pallas_call(
        functools.partial(send_kernel, depth),
        out_shape=jax.ShapeDtypeStruct((devices, planes * SUB + 1, 1, LANES), jnp.float32),
        in_specs=[vmem(), vmem(), vmem(), smem(), smem()],
        out_specs=vmem(),
        name="send",
    )(volume, all_steps, all_cols, materials, tf_table)
    recv = lax.all_to_all(blocks, ("view", "depth"), split_axis=0, concat_axis=0, tiled=True)

    maps = jnp.kron(jnp.eye(rows // edge, dtype=jnp.float32), row_interp[0].T)
    entry_own = lax.dynamic_slice_in_dim(entry[0].T, lax.axis_index("depth") * per, per, 0)
    image = pl.pallas_call(
        functools.partial(render_kernel, step_length),
        out_shape=jax.ShapeDtypeStruct((depth, rows // depth, LANES), jnp.float32),
        in_specs=[vmem()] * 3,
        out_specs=vmem(),
        scratch_shapes=[pltpu.VMEM((devices * planes * SUB, LANES), jnp.float32)],
        name="render",
    )(recv, maps, entry_own)
    turned = lax.all_to_all(image, "depth", split_axis=0, concat_axis=0, tiled=True)
    return pl.pallas_call(
        functools.partial(unpack_kernel, per),
        out_shape=jax.ShapeDtypeStruct((1, 3, rows // depth, lateral), jnp.float32),
        in_specs=[vmem()],
        out_specs=vmem(),
        name="unpack",
    )(turned)


def with_arrays(volume, all_steps, all_cols, row_interp, tf_table, materials, entry):
    views, steps, edge = all_steps.shape
    depth = lax.axis_size("depth")
    planes, lateral, span = volume.shape
    devices = views * depth
    per = lateral // depth
    rows = devices * planes
    tiles_z, tiles_y = materials.shape[:2]
    step_length = 2.0 / (steps * depth)
    cells = volume.reshape(planes, tiles_y, edge, depth, edge)
    first = jnp.einsum("pujbi,vsi->vpujbs", cells, all_steps, precision=HIGHEST)
    second = jnp.einsum("vpujbs,vcj->vpucbs", first, all_cols, precision=HIGHEST)
    second = second.reshape(views, planes, depth, per, depth, steps).transpose(0, 2, 1, 3, 4, 5)
    second = second.reshape(devices, planes * per * depth * steps)
    own = tf_table[materials[:, :, 0]].transpose(1, 0, 2).reshape(tiles_y, tiles_z * COEF)
    own = jnp.tile(jnp.repeat(own, edge // per, axis=0), (views, 1))
    payload = jnp.concatenate([second, own], axis=1)
    payload = jnp.pad(payload, ((0, 0), (0, -payload.shape[1] % LANES)))
    payload = payload.reshape(devices, -1, 1, LANES)
    recv = lax.all_to_all(payload, ("view", "depth"), split_axis=0, concat_axis=0, tiled=True)
    recv = recv.reshape(devices, -1)
    size = second.shape[1]
    coef = recv[:depth, size : size + tiles_z * COEF].reshape(depth, tiles_z, COEF)
    coef = jnp.repeat(coef.transpose(2, 1, 0), edge, axis=1)[:, :, None, :, None]
    third = recv[:, :size].reshape(tiles_z, edge, per, depth, steps)
    third = jnp.einsum("tkcbs,rk->trcbs", third, row_interp[0], precision=HIGHEST)
    samples = third.reshape(rows, per, depth, steps)
    entry_own = lax.dynamic_slice_in_dim(entry[0], lax.axis_index("depth") * per, per, 1)
    live = (entry_own[:, :, None] <= jnp.arange(depth)).astype(jnp.float32)
    tau = step_length * live[..., None] * jax.nn.softplus(coef[6] * samples + coef[7])
    flat = tau.reshape(rows, per, depth * steps)
    earlier = (jnp.cumsum(flat, axis=2) - flat).reshape(tau.shape)
    weights = jnp.exp(-earlier) * (1.0 - jnp.exp(-tau))
    emission = jax.nn.softplus(coef[0:3] * samples + coef[3:6])
    image = jnp.sum(weights * emission, axis=(3, 4))
    turned = lax.all_to_all(image, "depth", split_axis=1, concat_axis=2, tiled=True)
    return turned[None]


def shards(volume, step_weights, row_interp, col_interp, tf_table, materials, entry):
    views = lax.axis_size("view")
    depth = lax.axis_size("depth")
    all_steps = lax.all_gather(step_weights, "view", axis=0, tiled=True)
    all_cols = lax.all_gather(col_interp, "view", axis=0, tiled=True)
    planes, lateral, span = volume.shape
    steps, edge = step_weights.shape[1:]
    rows = views * depth * planes
    fits = (
        depth == SUB
        and steps == SUB
        and edge == LANES // 2
        and lateral == LANES
        and rows == LANES
        and views % 2 == 0
        and span == depth * edge
    )
    run = with_kernels if fits else with_arrays
    return run(volume, all_steps, all_cols, row_interp, tf_table, materials, entry)


def solution(mesh):
    placed = (
        P(("view", "depth"), None, None),
        P("view", None, None),
        P("view", None, None),
        P("view", None, None),
        P(),
        P(None, None, "depth"),
        P("view", None, None),
    )
    return jax.shard_map(
        shards,
        mesh=mesh,
        in_specs=placed,
        out_specs=P("view", None, "depth", None),
        check_vma=False,
    )
```

```python
import functools

import jax
import jax.numpy as jnp
from jax import lax
from jax.experimental import pallas as pl
from jax.experimental.pallas import tpu as pltpu
from jax.sharding import PartitionSpec as P

LANES = 128
SUB = 8
COEF = 8
HIGHEST = lax.Precision.HIGHEST
NT = (((1,), (1,)), ((), ()))
NN = (((1,), (0,)), ((), ()))


def split(x):
    hi = x.astype(jnp.bfloat16)
    return hi, (x - hi.astype(jnp.float32)).astype(jnp.bfloat16)


def dot3(a, b, dims):
    dot = functools.partial(
        lax.dot_general, dimension_numbers=dims, preferred_element_type=jnp.float32
    )
    return dot(a[0], b[0]) + (dot(a[0], b[1]) + dot(a[1], b[0]))


def softplus(v):
    e = jnp.exp(-jnp.abs(v))
    small = e * (1.0 - 0.5 * e)
    return jnp.maximum(v, 0.0) + jnp.where(e < 1e-4, small, jnp.log(1.0 + e))


def pack_kernel(steps_ref, cols_ref, out_ref, sems):
    steps = steps_ref.shape[1]
    copies = [
        pltpu.make_async_copy(steps_ref.at[0], out_ref.at[0, pl.ds(0, steps)], sems.at[0]),
        pltpu.make_async_copy(cols_ref.at[0], out_ref.at[0, pl.ds(steps, cols_ref.shape[1])], sems.at[1]),
    ]
    for copy in copies:
        copy.start()
    for copy in copies:
        copy.wait()


def prepare_kernel(
    depth_ref, classes_hbm, table_hbm, vol_hbm, row_hbm, entry_hbm,
    hi_ref, lo_ref, maps_hi_ref, maps_lo_ref, entry_own_ref, coef_ref,
    classes_ref, table_ref, vol_ref, row_ref, entry_ref, sems,
):
    planes, lateral, span = vol_ref.shape
    tiles_z, tiles_y = classes_ref.shape[0], classes_ref.shape[2]
    per = entry_own_ref.shape[0]
    pieces = [(vol_hbm.at[p], vol_ref.at[p]) for p in range(planes)]
    pieces += [(entry_hbm, entry_ref), (row_hbm, row_ref), (classes_hbm, classes_ref), (table_hbm, table_ref)]
    copies = [pltpu.make_async_copy(*piece, sems.at[n]) for n, piece in enumerate(pieces)]
    for copy in copies:
        copy.start()
    for copy in copies[planes:]:
        copy.wait()
    lane = lax.broadcasted_iota(jnp.int32, (1, LANES), 1)
    for u in range(tiles_y):
        row = jnp.zeros((1, LANES), jnp.float32)
        for t in range(tiles_z):
            for ch in range(COEF):
                row = jnp.where(lane == t * COEF + ch, table_ref[classes_ref[t, 0, u], ch], row)
        coef_ref[u : u + 1] = row
    turned = row_ref[0].T
    zero = jnp.zeros_like(turned)
    maps = jnp.concatenate(
        [jnp.concatenate([turned if i == t else zero for i in range(tiles_z)], axis=1) for t in range(tiles_z)],
        axis=0,
    )
    maps_hi_ref[...], maps_lo_ref[...] = split(maps)
    turned = entry_ref[0].astype(jnp.float32).T
    own = jnp.zeros((per, turned.shape[1]), jnp.float32)
    for d in range(turned.shape[0] // per):
        own = jnp.where(depth_ref[0] == d, turned[d * per : (d + 1) * per], own)
    entry_own_ref[...] = own.astype(jnp.int32)
    for p in range(planes):
        copies[p].wait()
        at = slice(p * lateral, (p + 1) * lateral)
        hi_ref[at], lo_ref[at] = split(vol_ref[p])


def send_kernel(depth, planes, view_ref, hi_ref, lo_ref, coef_ref, *refs):
    out_ref = refs[-1]
    map_refs = refs[:-1]
    views = len(map_refs)
    edge = map_refs[0].shape[2]
    steps = map_refs[0].shape[1] - edge
    lateral, span = hi_ref.shape[0] // planes, hi_ref.shape[1]
    bricks = span // edge
    tiles_y = lateral // edge
    per = lateral // depth
    view = [view_ref[0] ^ k for k in range(views)]

    weights = jnp.concatenate([ref[0, :steps] for ref in map_refs], axis=0)
    tiled = jnp.concatenate([weights] * bricks, axis=1)
    lane = lax.broadcasted_iota(jnp.int32, (bricks, span), 1)
    brick = lax.broadcasted_iota(jnp.int32, (bricks, span), 0)
    own = lane // edge == brick
    ray = jnp.where(own[None], tiled[:, None, :], 0.0).reshape(views * steps * bricks, span)
    first = dot3((hi_ref[...], lo_ref[...]), split(ray), NT)
    first_hi, first_lo = split(first)

    half = lax.broadcasted_iota(jnp.int32, (SUB, LANES), 1) < LANES // 2
    zero = jnp.zeros((edge, edge), jnp.float32)
    for pair in range(views // 2):
        rows = []
        for k in (2 * pair, 2 * pair + 1):
            c = map_refs[k][0, steps:]
            for tile in range(tiles_y):
                rows.append(jnp.concatenate([c if t == tile else zero for t in range(tiles_y)], axis=1))
        maps = split(jnp.concatenate(rows, axis=0))
        for plane in range(planes):
            at = slice(plane * lateral, (plane + 1) * lateral)
            to = slice(pair * LANES, (pair + 1) * LANES)
            second = dot3(maps, (first_hi[at, to], first_lo[at, to]), NN)
            for k in range(2):
                for d in range(depth):
                    base = k * lateral + d * per
                    a = second[base : base + SUB]
                    b = second[base + SUB : base + 2 * SUB]
                    if k == 0:
                        b = pltpu.roll(b, LANES // 2, 1)
                    else:
                        a = pltpu.roll(a, LANES // 2, 1)
                    block = jnp.where(half, a, b)
                    out_ref[view[2 * pair + k] * depth + d, plane * SUB : (plane + 1) * SUB, 0, :] = block
    for v in range(views):
        for d in range(depth):
            u = d * per // edge
            out_ref[v * depth + d, planes * SUB : planes * SUB + 1, 0, :] = coef_ref[u : u + 1]


def render_kernel(step_length, recv_ref, maps_hi_ref, maps_lo_ref, entry_ref, out_ref, cells):
    sources, rows_block = recv_ref.shape[:2]
    data = rows_block - 1
    columns, rows = entry_ref.shape
    bricks = steps = SUB
    for s in range(sources):
        cells[s * data : (s + 1) * data, :] = recv_ref[s, 0:data, 0, :]
    maps = (maps_hi_ref[...], maps_lo_ref[...])

    packed = jnp.concatenate([recv_ref[b, data : data + 1, 0, :] for b in range(bricks)], axis=0)
    lane = lax.broadcasted_iota(jnp.int32, (bricks, rows), 1)
    upper = lane >= rows // 2
    coef = []
    for ch in range(COEF):
        low = jnp.broadcast_to(packed[:, ch : ch + 1], (bricks, rows))
        high = jnp.broadcast_to(packed[:, COEF + ch : COEF + ch + 1], (bricks, rows))
        coef.append(jnp.where(upper, high, low))
    brick = lax.broadcasted_iota(jnp.int32, (bricks, rows), 0)

    shown = [[None] * columns for _ in range(3)]
    for x in range(SUB):
        planes = cells[pl.ds(x, rows, stride=SUB), :]
        samples = dot3(split(planes.T), maps, NN)
        for low in range(2):
            c = low * SUB + x
            live = jnp.where(entry_ref[c : c + 1, :] <= brick, step_length, 0.0)
            total = jnp.zeros((bricks, rows), jnp.float32)
            before = jnp.ones((bricks, rows), jnp.float32)
            colours = [jnp.zeros((bricks, rows), jnp.float32) for _ in range(3)]
            for s in range(steps):
                at = (low * steps + s) * bricks
                v = samples[at : at + bricks]
                total = total + live * softplus(coef[6] * v + coef[7])
                after = jnp.exp(-total)
                weight = before - after
                before = after
                for ch in range(3):
                    colours[ch] = colours[ch] + weight * softplus(coef[ch] * v + coef[3 + ch])
            front = total
            for shift in (1, 2, 4):
                front = front + jnp.where(brick >= shift, pltpu.roll(front, shift, 0), 0.0)
            reach = jnp.exp(total - front)
            for ch in range(3):
                shown[ch][c] = jnp.sum(reach * colours[ch], axis=0, keepdims=True)
    blank = jnp.zeros((LANES - 3 * columns, rows), jnp.float32)
    image = jnp.concatenate([r for ch in shown for r in ch] + [blank], axis=0)
    out_ref[...] = image.T.reshape(out_ref.shape)


def unpack_kernel(columns, recv_ref, out_ref):
    sources, rows, _ = recv_ref.shape
    owner = lax.broadcasted_iota(jnp.int32, (rows, LANES), 1) // columns
    for ch in range(3):
        out = jnp.zeros((rows, LANES), jnp.float32)
        for s in range(sources):
            moved = pltpu.roll(recv_ref[s], ((s - ch) * columns) % LANES, 1)
            out = jnp.where(owner == s, moved, out)
        out_ref[0, ch] = out


def small():
    return pltpu.CompilerParams(vmem_limit_bytes=16 * 1024 * 1024)


def vmem():
    return pl.BlockSpec(memory_space=pltpu.VMEM)


def hbm():
    return pl.BlockSpec(memory_space=pltpu.HBM)


def in_hbm(x):
    return pltpu.with_memory_space_constraint(x, pltpu.HBM)


def smem():
    return pl.BlockSpec(memory_space=pltpu.SMEM)


def with_kernels(volume, step_weights, row_interp, col_interp, tf_table, materials, entry):
    views = lax.axis_size("view")
    steps, edge = step_weights.shape[1:]
    depth = lax.axis_size("depth")
    planes, lateral, span = volume.shape
    devices = views * depth
    per = lateral // depth
    rows = devices * planes
    step_length = 2.0 / (steps * depth)
    tiles_y = lateral // edge
    depth_at = lax.axis_index("depth").reshape(1)
    own = pl.pallas_call(
        pack_kernel,
        out_shape=jax.ShapeDtypeStruct((1, steps + edge, edge), jnp.float32),
        in_specs=[hbm()] * 2,
        out_specs=vmem(),
        scratch_shapes=[pltpu.SemaphoreType.DMA((2,))],
        compiler_params=small(),
        name="pack",
    )(in_hbm(step_weights), in_hbm(col_interp))
    maps = [own] + [lax.ppermute(own, "view", [(i, i ^ k) for i in range(views)]) for k in range(1, views)]
    hi, lo, maps_hi, maps_lo, entry_own, coef = pl.pallas_call(
        prepare_kernel,
        out_shape=[
            jax.ShapeDtypeStruct((planes * lateral, span), jnp.bfloat16),
            jax.ShapeDtypeStruct((planes * lateral, span), jnp.bfloat16),
            jax.ShapeDtypeStruct((rows, rows), jnp.bfloat16),
            jax.ShapeDtypeStruct((rows, rows), jnp.bfloat16),
            jax.ShapeDtypeStruct((per, rows), jnp.int32),
            jax.ShapeDtypeStruct((tiles_y, LANES), jnp.float32),
        ],
        in_specs=[smem()] + [hbm()] * 5,
        out_specs=[vmem()] * 6,
        scratch_shapes=[
            pltpu.SMEM((materials.shape[0], 1, tiles_y), jnp.int32),
            pltpu.SMEM(tf_table.shape, jnp.float32),
            pltpu.VMEM(volume.shape, jnp.float32),
            pltpu.VMEM(row_interp.shape, jnp.float32),
            pltpu.VMEM(entry.shape, jnp.int32),
            pltpu.SemaphoreType.DMA((planes + 4,)),
        ],
        compiler_params=small(),
        cost_estimate=pl.CostEstimate(flops=2_000_000_000, bytes_accessed=4_000_000, transcendentals=0),
        name="prepare",
    )(depth_at, *map(in_hbm, (materials.transpose(0, 2, 1), tf_table, volume, row_interp, entry)))
    blocks = pl.pallas_call(
        functools.partial(send_kernel, depth, planes),
        out_shape=jax.ShapeDtypeStruct((devices, planes * SUB + 1, 1, LANES), jnp.float32),
        in_specs=[smem()] + [vmem()] * (3 + views),
        out_specs=vmem(),
        compiler_params=small(),
        name="send",
    )(lax.axis_index("view").reshape(1), hi, lo, coef, *maps)
    recv = lax.all_to_all(blocks, ("view", "depth"), split_axis=0, concat_axis=0, tiled=True)

    image = pl.pallas_call(
        functools.partial(render_kernel, step_length),
        out_shape=jax.ShapeDtypeStruct((depth, rows // depth, LANES), jnp.float32),
        in_specs=[vmem()] * 4,
        out_specs=vmem(),
        scratch_shapes=[pltpu.VMEM((devices * planes * SUB, LANES), jnp.float32)],
        compiler_params=small(),
        name="render",
    )(recv, maps_hi, maps_lo, entry_own)
    turned = lax.all_to_all(image, "depth", split_axis=0, concat_axis=0, tiled=True)
    return pl.pallas_call(
        functools.partial(unpack_kernel, per),
        out_shape=jax.ShapeDtypeStruct((1, 3, rows // depth, lateral), jnp.float32),
        in_specs=[vmem()],
        out_specs=vmem(),
        compiler_params=small(),
        name="unpack",
    )(turned)


def with_arrays(volume, step_weights, row_interp, col_interp, tf_table, materials, entry):
    all_steps = lax.all_gather(step_weights, "view", axis=0, tiled=True)
    all_cols = lax.all_gather(col_interp, "view", axis=0, tiled=True)
    views, steps, edge = all_steps.shape
    depth = lax.axis_size("depth")
    planes, lateral, span = volume.shape
    devices = views * depth
    per = lateral // depth
    rows = devices * planes
    tiles_z, tiles_y = materials.shape[:2]
    step_length = 2.0 / (steps * depth)
    cells = volume.reshape(planes, tiles_y, edge, depth, edge)
    first = jnp.einsum("pujbi,vsi->vpujbs", cells, all_steps, precision=HIGHEST)
    second = jnp.einsum("vpujbs,vcj->vpucbs", first, all_cols, precision=HIGHEST)
    second = second.reshape(views, planes, depth, per, depth, steps).transpose(0, 2, 1, 3, 4, 5)
    second = second.reshape(devices, planes * per * depth * steps)
    own = tf_table[materials[:, :, 0]].transpose(1, 0, 2).reshape(tiles_y, tiles_z * COEF)
    own = jnp.tile(jnp.repeat(own, edge // per, axis=0), (views, 1))
    payload = jnp.concatenate([second, own], axis=1)
    payload = jnp.pad(payload, ((0, 0), (0, -payload.shape[1] % LANES)))
    payload = payload.reshape(devices, -1, 1, LANES)
    recv = lax.all_to_all(payload, ("view", "depth"), split_axis=0, concat_axis=0, tiled=True)
    recv = recv.reshape(devices, -1)
    size = second.shape[1]
    coef = recv[:depth, size : size + tiles_z * COEF].reshape(depth, tiles_z, COEF)
    coef = jnp.repeat(coef.transpose(2, 1, 0), edge, axis=1)[:, :, None, :, None]
    third = recv[:, :size].reshape(tiles_z, edge, per, depth, steps)
    third = jnp.einsum("tkcbs,rk->trcbs", third, row_interp[0], precision=HIGHEST)
    samples = third.reshape(rows, per, depth, steps)
    entry_own = lax.dynamic_slice_in_dim(entry[0], lax.axis_index("depth") * per, per, 1)
    live = (entry_own[:, :, None] <= jnp.arange(depth)).astype(jnp.float32)
    tau = step_length * live[..., None] * jax.nn.softplus(coef[6] * samples + coef[7])
    flat = tau.reshape(rows, per, depth * steps)
    earlier = (jnp.cumsum(flat, axis=2) - flat).reshape(tau.shape)
    weights = jnp.exp(-earlier) * (1.0 - jnp.exp(-tau))
    emission = jax.nn.softplus(coef[0:3] * samples + coef[3:6])
    image = jnp.sum(weights * emission, axis=(3, 4))
    turned = lax.all_to_all(image, "depth", split_axis=1, concat_axis=2, tiled=True)
    return turned[None]


def shards(volume, step_weights, row_interp, col_interp, tf_table, materials, entry):
    views = lax.axis_size("view")
    depth = lax.axis_size("depth")
    planes, lateral, span = volume.shape
    steps, edge = step_weights.shape[1:]
    rows = views * depth * planes
    fits = (
        depth == SUB
        and steps == SUB
        and edge == LANES // 2
        and lateral == LANES
        and rows == LANES
        and views in (2, 4, 8)
        and span == depth * edge
    )
    run = with_kernels if fits else with_arrays
    return run(volume, step_weights, row_interp, col_interp, tf_table, materials, entry)


def solution(mesh):
    placed = (
        P(("view", "depth"), None, None),
        P("view", None, None),
        P("view", None, None),
        P("view", None, None),
        P(),
        P(None, None, "depth"),
        P("view", None, None),
    )
    return jax.shard_map(
        shards,
        mesh=mesh,
        in_specs=placed,
        out_specs=P("view", None, "depth", None),
        check_vma=False,
    )
```

```python
import functools

import jax
import jax.numpy as jnp
from jax import lax
from jax.experimental import pallas as pl
from jax.experimental.pallas import tpu as pltpu
from jax.sharding import PartitionSpec as P


LANES = 128
SUB = 8
COEF = 8
HIGHEST = lax.Precision.HIGHEST
NT = (((1,), (1,)), ((), ()))
NN = (((1,), (0,)), ((), ()))


def split(x):
    hi = x.astype(jnp.bfloat16)
    return hi, (x - hi.astype(jnp.float32)).astype(jnp.bfloat16)


def softplus(v):
    e = jnp.exp(-jnp.abs(v))
    small = e * (1.0 - 0.5 * e)
    return jnp.maximum(v, 0.0) + jnp.where(e < 1e-4, small, jnp.log(1.0 + e))


def pack_kernel(steps_hbm, cols_hbm, out_ref, steps_ref, cols_ref, sems):
    copies = [
        pltpu.make_async_copy(cols_hbm, cols_ref, sems.at[0]),
        pltpu.make_async_copy(steps_hbm, steps_ref, sems.at[1]),
    ]
    for copy in copies:
        copy.start()
    for copy in copies:
        copy.wait()
    edge = cols_ref.shape[1]
    out_ref[0, : edge // 2] = jnp.concatenate([cols_ref[0, : edge // 2], cols_ref[0, edge // 2 :]], axis=1)
    out_ref[0, edge // 2 :] = jnp.concatenate([steps_ref[0], steps_ref[0]], axis=1)


def prepare_kernel(
    order, depth_ref, classes_hbm, table_hbm, vol_hbm, row_hbm, entry_hbm,
    hi_ref, lo_ref, maps_hi_ref, maps_lo_ref, entry_own_ref, coef_ref,
    classes_ref, table_ref, vol_ref, row_ref, entry_ref, turned_ref, moved_ref, sems,
):
    planes, lateral, _ = vol_ref.shape
    tiles_z, tiles_y = classes_ref.shape[0], classes_ref.shape[2]
    per = entry_own_ref.shape[0]
    pieces = [(vol_hbm.at[p], vol_ref.at[p]) for p in range(planes)]
    pieces += [(entry_hbm, entry_ref), (row_hbm, row_ref), (classes_hbm, classes_ref), (table_hbm, table_ref)]
    copies = [pltpu.make_async_copy(*piece, sems.at[n]) for n, piece in enumerate(pieces)]
    for copy in copies:
        copy.start()
    for copy in copies[planes:]:
        copy.wait()
    lane = lax.broadcasted_iota(jnp.int32, (1, LANES), 1)
    for u in range(tiles_y):
        row = jnp.zeros((1, LANES), jnp.float32)
        for t in range(tiles_z):
            for ch in range(COEF):
                row = jnp.where(lane == t * COEF + ch, table_ref[classes_ref[t, 0, u], ch], row)
        coef_ref[u : u + 1] = row
    turned = row_ref[0].T
    zero = jnp.zeros_like(turned)
    maps = jnp.concatenate(
        [jnp.concatenate([turned if i == t else zero for i in range(tiles_z)], axis=1) for t in range(tiles_z)],
        axis=0,
    )
    turned_ref[...] = maps
    for p in range(planes):
        for n, device in enumerate(order):
            to, at = p * len(order) + n, device * planes + p
            moved_ref[to : to + 1] = turned_ref[at : at + 1]
    maps_hi_ref[...], maps_lo_ref[...] = split(moved_ref[...])
    turned = entry_ref[0].astype(jnp.float32).T
    own = jnp.zeros((per, turned.shape[1]), jnp.float32)
    for d in range(turned.shape[0] // per):
        own = jnp.where(depth_ref[0] == d, turned[d * per : (d + 1) * per], own)
    entry_own_ref[...] = own.astype(jnp.int32)
    for p in range(planes):
        copies[p].wait()
        at = slice(p * lateral, (p + 1) * lateral)
        hi_ref[at], lo_ref[at] = split(vol_ref[p])


def send_kernel(order, depth, planes, pair, view_ref, hi_ref, lo_ref, coef_ref, *refs):
    out_ref = refs[-1]
    map_refs = refs[:2]
    edge = map_refs[0].shape[2] // 2
    lateral, span = hi_ref.shape[0] // planes, hi_ref.shape[1]
    bricks = span // edge
    per = lateral // depth
    block_rows = planes * SUB + 1
    views = len(order) // depth
    view = [view_ref[0] ^ (2 * pair + k) for k in range(2)]

    def first_row(k, d):
        row = order.index(d) * block_rows
        for v in range(1, views):
            row = jnp.where(view[k] == v, order.index(v * depth + d) * block_rows, row)
        return row

    starts = [[first_row(k, d) for d in range(depth)] for k in range(2)]

    weights = jnp.concatenate([ref[0, edge // 2 :] for ref in map_refs], axis=0)
    tiled = jnp.concatenate([weights] * (span // LANES), axis=1)
    lane = lax.broadcasted_iota(jnp.int32, (bricks, span), 1)
    brick = lax.broadcasted_iota(jnp.int32, (bricks, span), 0)
    own = lane // edge == brick
    ray = jnp.where(own[None], tiled[:, None, :], 0.0).reshape(weights.shape[0] * bricks, span)
    ray_hi, ray_lo = split(ray)
    both = lax.dot_general(
        hi_ref[...], jnp.concatenate([ray_hi, ray_lo], axis=0), NT, preferred_element_type=jnp.float32
    )
    first = both[:, :LANES] + (
        both[:, LANES:] + lax.dot_general(lo_ref[...], ray_hi, NT, preferred_element_type=jnp.float32)
    )
    first_hi, first_lo = split(first)

    half = lax.broadcasted_iota(jnp.int32, (SUB, LANES), 1) < edge
    left = lax.broadcasted_iota(jnp.int32, (edge // 2, LANES), 1) < edge
    rows = []
    for ref in map_refs:
        c = ref[0, : edge // 2]
        turned = pltpu.roll(c, edge, 1)
        rows += [jnp.where(left, c, 0.0), jnp.where(left, turned, 0.0)]
        rows += [jnp.where(left, 0.0, turned), jnp.where(left, 0.0, c)]
    maps_hi, maps_lo = split(jnp.concatenate(rows, axis=0))
    maps = jnp.concatenate([maps_hi, maps_lo], axis=1)
    for couple in range(planes // 2):
        at = [slice((2 * couple + i) * lateral, (2 * couple + i + 1) * lateral) for i in range(2)]
        high = jnp.concatenate([first_hi[i] for i in at], axis=1)
        low = jnp.concatenate([first_lo[i] for i in at], axis=1)
        second = lax.dot_general(
            maps, jnp.concatenate([high, high], axis=0), NN, preferred_element_type=jnp.float32
        ) + lax.dot_general(maps_hi, low, NN, preferred_element_type=jnp.float32)
        for i in range(2):
            plane = 2 * couple + i
            for k in range(2):
                for d in range(depth):
                    base = k * lateral + d * per
                    a = second[base : base + SUB, i * LANES : (i + 1) * LANES]
                    b = second[base + SUB : base + 2 * SUB, i * LANES : (i + 1) * LANES]
                    if k == 0:
                        b = pltpu.roll(b, edge, 1)
                    else:
                        a = pltpu.roll(a, edge, 1)
                    at_row = starts[k][d] + plane * SUB
                    out_ref[pl.ds(at_row, SUB), :] = jnp.where(half, a, b)
    for k in range(2):
        for d in range(depth):
            u = d * per // edge
            at_row = starts[k][d] + block_rows - 1
            out_ref[pl.ds(at_row, 1), :] = coef_ref[u : u + 1]


def render_kernel(step_length, planes, order, turn, recv_ref, maps_hi_ref, maps_lo_ref, entry_ref, out_ref):
    block_rows = planes * SUB + 1
    sources = recv_ref.shape[0] // block_rows
    columns, rows = entry_ref.shape
    bricks = steps = SUB
    maps_hi = maps_hi_ref[...]
    maps = jnp.concatenate([maps_hi, maps_hi], axis=0)
    maps_lo = maps_lo_ref[...]

    ends = [(order.index(b) + 1) * block_rows for b in range(bricks)]
    packed = jnp.concatenate([recv_ref[end - 1 : end] for end in ends], axis=0)
    lane = lax.broadcasted_iota(jnp.int32, (bricks, rows), 1)
    upper = lane >= rows // 2
    coef = []
    for ch in range(COEF):
        low = jnp.broadcast_to(packed[:, ch : ch + 1], (bricks, rows))
        high = jnp.broadcast_to(packed[:, COEF + ch : COEF + ch + 1], (bricks, rows))
        coef.append(jnp.where(upper, high, low))
    brick = lax.broadcasted_iota(jnp.int32, (bricks, rows), 0)

    shown = [[None] * columns for _ in range(3)]
    for x in range(SUB):
        cells = jnp.concatenate(
            [recv_ref[pl.ds(p * SUB + x, sources, stride=block_rows), :] for p in range(planes)], axis=0
        )
        high, low = split(cells.T)
        samples = lax.dot_general(
            jnp.concatenate([high, low], axis=1), maps, NN, preferred_element_type=jnp.float32
        ) + lax.dot_general(high, maps_lo, NN, preferred_element_type=jnp.float32)
        for m in range(2):
            c = m * SUB + x
            live = jnp.where(entry_ref[c : c + 1, :] <= brick, step_length, 0.0)
            total = jnp.zeros((bricks, rows), jnp.float32)
            before = jnp.ones((bricks, rows), jnp.float32)
            colours = [jnp.zeros((bricks, rows), jnp.float32) for _ in range(3)]
            for s in range(steps):
                at = (m * steps + s) * bricks
                v = samples[at : at + bricks]
                total = total + live * softplus(coef[6] * v + coef[7])
                after = jnp.exp(-total)
                weight = before - after
                before = after
                for ch in range(3):
                    colours[ch] = colours[ch] + weight * softplus(coef[ch] * v + coef[3 + ch])
            front = total
            for shift in (1, 2, 4):
                front = front + jnp.where(brick >= shift, pltpu.roll(front, shift, 0), 0.0)
            reach = jnp.exp(total - front)
            for ch in range(3):
                shown[ch][c] = jnp.sum(reach * colours[ch], axis=0, keepdims=True)
    blank = jnp.zeros((LANES // 2 - 3 * columns, rows), jnp.float32)
    image = jnp.concatenate([r for ch in shown for r in ch] + [blank], axis=0)
    image = jnp.concatenate([image, image], axis=0).T
    left = lax.broadcasted_iota(jnp.int32, (SUB, LANES), 1) < LANES // 2
    for n, d in enumerate(turn):
        at = d * 2 * SUB
        out_ref[n] = jnp.where(left, image[at : at + SUB], image[at + SUB : at + 2 * SUB])


def unpack_kernel(columns, turn, recv_ref, out_ref):
    owner = lax.broadcasted_iota(jnp.int32, (SUB, LANES), 1) // columns
    for ch in range(3):
        for h in range(2):
            out = jnp.zeros((SUB, LANES), jnp.float32)
            for n, s in enumerate(turn):
                moved = pltpu.roll(recv_ref[n], ((s - ch) * columns - h * (LANES // 2)) % LANES, 1)
                out = jnp.where(owner == s, moved, out)
            out_ref[0, ch, h * SUB : (h + 1) * SUB] = out


def small():
    return pltpu.CompilerParams(vmem_limit_bytes=16 * 1024 * 1024)


def orders(views, depth):
    order = [v * depth + z * 2 + y for y in range(2) for v in range(views) for z in range(depth // 2)]
    first = depth // 2 + 1
    return order, list(range(first, depth)) + list(range(first))


def vmem():
    return pl.BlockSpec(memory_space=pltpu.VMEM)


def hbm():
    return pl.BlockSpec(memory_space=pltpu.HBM)


def in_hbm(x):
    return pltpu.with_memory_space_constraint(x, pltpu.HBM)


def smem():
    return pl.BlockSpec(memory_space=pltpu.SMEM)


def with_kernels(volume, step_weights, row_interp, col_interp, tf_table, materials, entry):
    views = lax.axis_size("view")
    steps, edge = step_weights.shape[1:]
    depth = lax.axis_size("depth")
    planes, lateral, span = volume.shape
    devices = views * depth
    per = lateral // depth
    rows = devices * planes
    step_length = 2.0 / (steps * depth)
    tiles_y = lateral // edge
    block_rows = planes * SUB + 1
    order, turn = orders(views, depth)
    depth_at = lax.axis_index("depth").reshape(1)
    own = pl.pallas_call(
        pack_kernel,
        out_shape=jax.ShapeDtypeStruct((1, edge // 2 + steps, 2 * edge), jnp.float32),
        in_specs=[hbm()] * 2,
        out_specs=vmem(),
        scratch_shapes=[
            pltpu.VMEM(step_weights.shape, jnp.float32),
            pltpu.VMEM(col_interp.shape, jnp.float32),
            pltpu.SemaphoreType.DMA((2,)),
        ],
        compiler_params=small(),
        name="pack",
    )(in_hbm(step_weights), in_hbm(col_interp))
    maps = [own]
    for k in range(1, views):
        maps.append(lax.ppermute(own, "view", [(i, i ^ k) for i in range(views)]))
    hi, lo, maps_hi, maps_lo, entry_own, coef = pl.pallas_call(
        functools.partial(prepare_kernel, order),
        out_shape=[
            jax.ShapeDtypeStruct((planes * lateral, span), jnp.bfloat16),
            jax.ShapeDtypeStruct((planes * lateral, span), jnp.bfloat16),
            jax.ShapeDtypeStruct((rows, rows), jnp.bfloat16),
            jax.ShapeDtypeStruct((rows, rows), jnp.bfloat16),
            jax.ShapeDtypeStruct((per, rows), jnp.int32),
            jax.ShapeDtypeStruct((tiles_y, LANES), jnp.float32),
        ],
        in_specs=[smem()] + [hbm()] * 5,
        out_specs=[vmem()] * 6,
        scratch_shapes=[
            pltpu.SMEM((materials.shape[0], 1, tiles_y), jnp.int32),
            pltpu.SMEM(tf_table.shape, jnp.float32),
            pltpu.VMEM(volume.shape, jnp.float32),
            pltpu.VMEM(row_interp.shape, jnp.float32),
            pltpu.VMEM(entry.shape, jnp.int32),
            pltpu.VMEM((rows, rows), jnp.float32),
            pltpu.VMEM((rows, rows), jnp.float32),
            pltpu.SemaphoreType.DMA((planes + 4,)),
        ],
        compiler_params=small(),
        cost_estimate=pl.CostEstimate(flops=2_000_000_000, bytes_accessed=4_000_000, transcendentals=0),
        name="prepare",
    )(depth_at, *map(in_hbm, (materials.transpose(0, 2, 1), tf_table, volume, row_interp, entry)))
    view_at = lax.axis_index("view").reshape(1)
    blocks = []
    for pair in range(views // 2):
        blocks = [
            pl.pallas_call(
                functools.partial(send_kernel, order, depth, planes, pair),
                out_shape=jax.ShapeDtypeStruct((devices * block_rows, LANES), jnp.float32),
                in_specs=[smem()] + [vmem()] * (5 + len(blocks)),
                out_specs=vmem(),
                input_output_aliases={6: 0} if blocks else {},
                compiler_params=small(),
                cost_estimate=pl.CostEstimate(flops=1_000_000_000, bytes_accessed=2_000_000, transcendentals=0),
            )(view_at, hi, lo, coef, *maps[2 * pair : 2 * pair + 2], *blocks)
        ]
    blocks = blocks[0]
    blocks = blocks.reshape(devices, block_rows, 1, LANES)
    recv = lax.all_to_all(blocks, ("view", "depth"), split_axis=0, concat_axis=0, tiled=True, axis_index_groups=[order])
    recv = recv.reshape(devices * block_rows, LANES)
    image = pl.pallas_call(
        functools.partial(render_kernel, step_length, planes, order, turn),
        out_shape=jax.ShapeDtypeStruct((depth, SUB, LANES), jnp.float32),
        in_specs=[vmem()] * 4,
        out_specs=vmem(),
        compiler_params=small(),
        name="render",
    )(recv, maps_hi, maps_lo, entry_own)
    turned = lax.all_to_all(image, "depth", split_axis=0, concat_axis=0, tiled=True, axis_index_groups=[turn])
    return pl.pallas_call(
        functools.partial(unpack_kernel, per, turn),
        out_shape=jax.ShapeDtypeStruct((1, 3, rows // depth, lateral), jnp.float32),
        in_specs=[vmem()],
        out_specs=vmem(),
        compiler_params=small(),
        name="unpack",
    )(turned)


def with_arrays(volume, step_weights, row_interp, col_interp, tf_table, materials, entry):
    all_steps = lax.all_gather(step_weights, "view", axis=0, tiled=True)
    all_cols = lax.all_gather(col_interp, "view", axis=0, tiled=True)
    views, steps, edge = all_steps.shape
    depth = lax.axis_size("depth")
    planes, lateral, _ = volume.shape
    devices = views * depth
    per = lateral // depth
    rows = devices * planes
    tiles_z, tiles_y = materials.shape[:2]
    step_length = 2.0 / (steps * depth)
    cells = volume.reshape(planes, tiles_y, edge, depth, edge)
    first = jnp.einsum("pujbi,vsi->vpujbs", cells, all_steps, precision=HIGHEST)
    second = jnp.einsum("vpujbs,vcj->vpucbs", first, all_cols, precision=HIGHEST)
    second = second.reshape(views, planes, depth, per, depth, steps).transpose(0, 2, 1, 3, 4, 5)
    second = second.reshape(devices, planes * per * depth * steps)
    own = tf_table[materials[:, :, 0]].transpose(1, 0, 2).reshape(tiles_y, tiles_z * COEF)
    own = jnp.tile(jnp.repeat(own, edge // per, axis=0), (views, 1))
    payload = jnp.concatenate([second, own], axis=1)
    payload = jnp.pad(payload, ((0, 0), (0, -payload.shape[1] % LANES)))
    payload = payload.reshape(devices, -1, 1, LANES)
    recv = lax.all_to_all(payload, ("view", "depth"), split_axis=0, concat_axis=0, tiled=True)
    recv = recv.reshape(devices, -1)
    size = second.shape[1]
    coef = recv[:depth, size : size + tiles_z * COEF].reshape(depth, tiles_z, COEF)
    coef = jnp.repeat(coef.transpose(2, 1, 0), edge, axis=1)[:, :, None, :, None]
    third = recv[:, :size].reshape(tiles_z, edge, per, depth, steps)
    third = jnp.einsum("tkcbs,rk->trcbs", third, row_interp[0], precision=HIGHEST)
    samples = third.reshape(rows, per, depth, steps)
    entry_own = lax.dynamic_slice_in_dim(entry[0], lax.axis_index("depth") * per, per, 1)
    live = (entry_own[:, :, None] <= jnp.arange(depth)).astype(jnp.float32)
    tau = step_length * live[..., None] * jax.nn.softplus(coef[6] * samples + coef[7])
    flat = tau.reshape(rows, per, depth * steps)
    earlier = (jnp.cumsum(flat, axis=2) - flat).reshape(tau.shape)
    weights = jnp.exp(-earlier) * (1.0 - jnp.exp(-tau))
    emission = jax.nn.softplus(coef[0:3] * samples + coef[3:6])
    image = jnp.sum(weights * emission, axis=(3, 4))
    turned = lax.all_to_all(image, "depth", split_axis=1, concat_axis=2, tiled=True)
    return turned[None]


def shards(volume, step_weights, row_interp, col_interp, tf_table, materials, entry):
    views = lax.axis_size("view")
    depth = lax.axis_size("depth")
    planes, lateral, span = volume.shape
    steps, edge = step_weights.shape[1:]
    rows = views * depth * planes
    fits = (
        depth == SUB
        and steps == SUB
        and edge == LANES // 2
        and lateral == LANES
        and rows == LANES
        and views in (2, 4, 8)
        and span == depth * edge
    )
    run = with_kernels if fits else with_arrays
    return run(volume, step_weights, row_interp, col_interp, tf_table, materials, entry)


def solution(mesh):
    placed = (
        P(("view", "depth"), None, None),
        P("view", None, None),
        P("view", None, None),
        P("view", None, None),
        P(),
        P(None, None, "depth"),
        P("view", None, None),
    )
    return jax.shard_map(
        shards,
        mesh=mesh,
        in_specs=placed,
        out_specs=P("view", None, "depth", None),
        check_vma=False,
    )
```

```python
import functools

import jax
import jax.numpy as jnp
from jax import lax
from jax.experimental import pallas as pl
from jax.experimental.pallas import tpu as pltpu
from jax.sharding import PartitionSpec as P


LANES = 128
SUB = 8
COEF = 8
CORES = 2
HIGHEST = lax.Precision.HIGHEST
NT = (((1,), (1,)), ((), ()))
NN = (((1,), (0,)), ((), ()))


def split(x):
    hi = x.astype(jnp.bfloat16)
    return hi, (x - hi.astype(jnp.float32)).astype(jnp.bfloat16)


def softplus(v):
    e = jnp.exp(-jnp.abs(v))
    small = e * (1.0 - 0.5 * e)
    return jnp.maximum(v, 0.0) + jnp.where(e < 1e-4, small, jnp.log(1.0 + e))


def fetch_kernel(
    steps_hbm, cols_hbm, classes_hbm, table_hbm, vol_hbm, row_hbm, entry_hbm,
    packed_ref, vol_ref, row_ref, entry_ref, coef_ref,
    steps_ref, cols_ref, classes_ref, table_ref, sems,
):
    pieces = [
        (cols_hbm, cols_ref), (steps_hbm, steps_ref), (classes_hbm, classes_ref), (table_hbm, table_ref),
        (row_hbm, row_ref), (entry_hbm, entry_ref),
    ]
    pieces += [(vol_hbm.at[p], vol_ref.at[p]) for p in range(vol_ref.shape[0])]
    copies = [pltpu.make_async_copy(*piece, sems.at[n]) for n, piece in enumerate(pieces)]
    for copy in copies:
        copy.start()
    for copy in copies[:4]:
        copy.wait()
    edge = cols_ref.shape[1]
    packed_ref[0, : edge // 2] = jnp.concatenate([cols_ref[0, : edge // 2], cols_ref[0, edge // 2 :]], axis=1)
    packed_ref[0, edge // 2 :] = jnp.concatenate([steps_ref[0], steps_ref[0]], axis=1)
    lane = lax.broadcasted_iota(jnp.int32, (1, LANES), 1)
    for u in range(classes_ref.shape[2]):
        row = jnp.zeros((1, LANES), jnp.float32)
        for t in range(classes_ref.shape[0]):
            for ch in range(COEF):
                row = jnp.where(lane == t * COEF + ch, table_ref[classes_ref[t, 0, u], ch], row)
        coef_ref[u : u + 1] = row
    for copy in copies[4:]:
        copy.wait()


def prepare_kernel(
    order, planes, view_ref, depth_ref, vol_ref, row_ref, entry_ref,
    hi_ref, lo_ref, maps_hi_ref, maps_lo_ref, entry_own_ref,
    turned_ref, moved_ref,
):
    per = entry_own_ref.shape[0]
    turned = row_ref[0].T
    zero = jnp.zeros_like(turned)
    tiles_z = turned_ref.shape[0] // turned.shape[0]
    turned_ref[...] = jnp.concatenate(
        [jnp.concatenate([turned if i == t else zero for i in range(tiles_z)], axis=1) for t in range(tiles_z)],
        axis=0,
    )
    core = view_ref[0] % CORES
    depth = entry_ref.shape[2] // per
    for swapped in range(CORES):
        slab = (core ^ swapped) * depth * planes
        for p in range(planes):
            for n, (chip, d) in enumerate(order):
                to = (swapped * planes + p) * len(order) + n
                at = slab + (chip * CORES * depth + d) * planes + p
                moved_ref[to : to + 1] = turned_ref[pl.ds(at, 1), :]
    maps_hi_ref[...], maps_lo_ref[...] = split(moved_ref[...])
    turned = entry_ref[0].astype(jnp.float32).T
    own = jnp.zeros((per, turned.shape[1]), jnp.float32)
    for d in range(depth):
        own = jnp.where(depth_ref[0] == d, turned[d * per : (d + 1) * per], own)
    entry_own_ref[...] = own.astype(jnp.int32)
    halve_kernel(vol_ref, hi_ref, lo_ref)


def halve_kernel(vol_ref, hi_ref, lo_ref):
    lateral = vol_ref.shape[1]
    for p in range(vol_ref.shape[0]):
        at = slice(p * lateral, (p + 1) * lateral)
        hi_ref[at], lo_ref[at] = split(vol_ref[p])


def send_kernel(order, depth, planes, flip, view_ref, hi_ref, lo_ref, hi_swapped_ref, lo_swapped_ref, coef_ref, map_ref, *refs):
    out_ref = refs[-1]
    edge = map_ref.shape[2] // 2
    lateral, span = hi_ref.shape[0] // planes, hi_ref.shape[1]
    bricks = span // edge
    per = lateral // depth
    block_rows = CORES * planes * SUB + 1
    chip = (view_ref[0] // CORES) ^ flip
    starts = []
    for d in range(depth):
        row = order.index((0, d)) * block_rows
        for x in range(1, len(order) // depth):
            row = jnp.where(chip == x, order.index((x, d)) * block_rows, row)
        starts.append(row)

    weights = map_ref[0, edge // 2 :]
    tiled = jnp.concatenate([weights] * (span // LANES), axis=1)
    lane = lax.broadcasted_iota(jnp.int32, (bricks, span), 1)
    brick = lax.broadcasted_iota(jnp.int32, (bricks, span), 0)
    own = lane // edge == brick
    ray = jnp.where(own[None], tiled[:, None, :], 0.0).reshape(weights.shape[0] * bricks, span)
    ray_hi, ray_lo = split(ray)
    ray_hi = jnp.concatenate([ray_hi, ray_hi], axis=0)
    ray_both = jnp.concatenate([ray_hi, ray_lo, ray_lo], axis=0)

    half = lax.broadcasted_iota(jnp.int32, (SUB, LANES), 1) < edge
    left = lax.broadcasted_iota(jnp.int32, (edge // 2, LANES), 1) < edge
    c = map_ref[0, : edge // 2]
    turned = pltpu.roll(c, edge, 1)
    rows = [jnp.where(left, c, 0.0), jnp.where(left, turned, 0.0)]
    rows += [jnp.where(left, 0.0, turned), jnp.where(left, 0.0, c)]
    maps_hi, maps_lo = split(jnp.concatenate(rows, axis=0))
    maps = jnp.concatenate([maps_hi, maps_lo], axis=1)
    for swapped, (high_ref, low_ref) in enumerate(((hi_ref, lo_ref), (hi_swapped_ref, lo_swapped_ref))):
        both = lax.dot_general(high_ref[...], ray_both, NT, preferred_element_type=jnp.float32)
        first = both[:, :LANES] + (
            both[:, LANES:] + lax.dot_general(low_ref[...], ray_hi, NT, preferred_element_type=jnp.float32)
        )
        first_hi, first_lo = split(first)
        for couple in range(planes // 2):
            at = [slice((2 * couple + i) * lateral, (2 * couple + i + 1) * lateral) for i in range(2)]
            high = jnp.concatenate([first_hi[i] for i in at], axis=1)
            low = jnp.concatenate([first_lo[i] for i in at], axis=1)
            second = lax.dot_general(
                maps, jnp.concatenate([high, high], axis=0), NN, preferred_element_type=jnp.float32
            ) + lax.dot_general(maps_hi, low, NN, preferred_element_type=jnp.float32)
            for i in range(2):
                plane = swapped * planes + 2 * couple + i
                for d in range(depth):
                    base = d * per
                    a = second[base : base + SUB, i * LANES : (i + 1) * LANES]
                    b = second[base + SUB : base + 2 * SUB, i * LANES : (i + 1) * LANES]
                    out_ref[pl.ds(starts[d] + plane * SUB, SUB), :] = jnp.where(half, a, b)
    for d in range(depth):
        u = d * per // edge
        out_ref[pl.ds(starts[d] + block_rows - 1, 1), :] = coef_ref[u : u + 1]


def render_kernel(step_length, planes, order, turn, recv_ref, maps_hi_ref, maps_lo_ref, entry_ref, out_ref):
    block_rows = planes * SUB + 1
    sources = len(order)
    columns, rows = entry_ref.shape
    bricks = steps = SUB
    maps_hi = maps_hi_ref[...]
    maps = jnp.concatenate([maps_hi, maps_hi], axis=0)
    maps_lo = maps_lo_ref[...]

    ends = [(order.index((0, b)) + 1) * block_rows for b in range(bricks)]
    packed = jnp.concatenate([recv_ref[end - 1 : end] for end in ends], axis=0)
    lane = lax.broadcasted_iota(jnp.int32, (bricks, rows), 1)
    upper = lane >= rows // 2
    coef = []
    for ch in range(COEF):
        low = jnp.broadcast_to(packed[:, ch : ch + 1], (bricks, rows))
        high = jnp.broadcast_to(packed[:, COEF + ch : COEF + ch + 1], (bricks, rows))
        coef.append(jnp.where(upper, high, low))
    brick = lax.broadcasted_iota(jnp.int32, (bricks, rows), 0)

    shown = [[None] * columns for _ in range(3)]
    for x in range(SUB):
        cells = jnp.concatenate(
            [recv_ref[pl.ds(p * SUB + x, sources, stride=block_rows), :] for p in range(planes)], axis=0
        )
        high, low = split(cells.T)
        samples = lax.dot_general(
            jnp.concatenate([high, low], axis=1), maps, NN, preferred_element_type=jnp.float32
        ) + lax.dot_general(high, maps_lo, NN, preferred_element_type=jnp.float32)
        for m in range(2):
            c = m * SUB + x
            live = jnp.where(entry_ref[c : c + 1, :] <= brick, step_length, 0.0)
            total = jnp.zeros((bricks, rows), jnp.float32)
            before = jnp.ones((bricks, rows), jnp.float32)
            colours = [jnp.zeros((bricks, rows), jnp.float32) for _ in range(3)]
            for s in range(steps):
                at = (m * steps + s) * bricks
                v = samples[at : at + bricks]
                total = total + live * softplus(coef[6] * v + coef[7])
                after = jnp.exp(-total)
                weight = before - after
                before = after
                for ch in range(3):
                    colours[ch] = colours[ch] + weight * softplus(coef[ch] * v + coef[3 + ch])
            front = total
            for shift in (1, 2, 4):
                front = front + jnp.where(brick >= shift, pltpu.roll(front, shift, 0), 0.0)
            reach = jnp.exp(total - front)
            for ch in range(3):
                shown[ch][c] = jnp.sum(reach * colours[ch], axis=0, keepdims=True)
    blank = jnp.zeros((LANES // 2 - 3 * columns, rows), jnp.float32)
    image = jnp.concatenate([r for ch in shown for r in ch] + [blank], axis=0)
    image = jnp.concatenate([image, image], axis=0).T
    left = lax.broadcasted_iota(jnp.int32, (SUB, LANES), 1) < LANES // 2
    for n, d in enumerate(turn):
        at = d * 2 * SUB
        out_ref[n] = jnp.where(left, image[at : at + SUB], image[at + SUB : at + 2 * SUB])


def unpack_kernel(columns, turn, recv_ref, out_ref):
    owner = lax.broadcasted_iota(jnp.int32, (SUB, LANES), 1) // columns
    for ch in range(3):
        for h in range(2):
            out = jnp.zeros((SUB, LANES), jnp.float32)
            for n, s in enumerate(turn):
                moved = pltpu.roll(recv_ref[n], ((s - ch) * columns - h * (LANES // 2)) % LANES, 1)
                out = jnp.where(owner == s, moved, out)
            out_ref[0, ch, h * SUB : (h + 1) * SUB] = out


def small():
    return pltpu.CompilerParams(vmem_limit_bytes=16 * 1024 * 1024)


def orders(views, depth):
    chips = views // CORES
    order = [(x, z * 2 + y) for y in range(2) for x in range(chips) for z in range(depth // 2)]
    first = order.index((chips - 1, depth // 2 + 1))
    turn = depth // 2 + 1
    return order[first:] + order[:first], list(range(turn, depth)) + list(range(turn))


def vmem():
    return pl.BlockSpec(memory_space=pltpu.VMEM)


def hbm():
    return pl.BlockSpec(memory_space=pltpu.HBM)


def in_hbm(x):
    return pltpu.with_memory_space_constraint(x, pltpu.HBM)


def smem():
    return pl.BlockSpec(memory_space=pltpu.SMEM)


def with_kernels(volume, step_weights, row_interp, col_interp, tf_table, materials, entry):
    views = lax.axis_size("view")
    steps, edge = step_weights.shape[1:]
    depth = lax.axis_size("depth")
    planes, lateral, span = volume.shape
    devices = views * depth
    per = lateral // depth
    rows = devices * planes
    step_length = 2.0 / (steps * depth)
    tiles_y = lateral // edge
    block_rows = CORES * planes * SUB + 1
    order, turn = orders(views, depth)
    groups = [[(x * CORES + core) * depth + d for x, d in order] for core in range(CORES)]
    depth_at = lax.axis_index("depth").reshape(1)
    view_at = lax.axis_index("view").reshape(1)
    slab = lax.ppermute(volume, "view", [(i, i ^ 1) for i in range(views)])
    own, vol, row, entry_all, coef = pl.pallas_call(
        fetch_kernel,
        out_shape=[
            jax.ShapeDtypeStruct((1, edge // 2 + steps, 2 * edge), jnp.float32),
            jax.ShapeDtypeStruct(volume.shape, volume.dtype),
            jax.ShapeDtypeStruct(row_interp.shape, row_interp.dtype),
            jax.ShapeDtypeStruct(entry.shape, entry.dtype),
            jax.ShapeDtypeStruct((tiles_y, LANES), jnp.float32),
        ],
        in_specs=[hbm()] * 7,
        out_specs=[vmem()] * 5,
        scratch_shapes=[
            pltpu.VMEM(step_weights.shape, jnp.float32),
            pltpu.VMEM(col_interp.shape, jnp.float32),
            pltpu.SMEM((materials.shape[0], 1, tiles_y), jnp.int32),
            pltpu.SMEM(tf_table.shape, jnp.float32),
            pltpu.SemaphoreType.DMA((planes + 6,)),
        ],
        compiler_params=small(),
        name="fetch",
    )(*map(in_hbm, (step_weights, col_interp, materials.transpose(0, 2, 1), tf_table, volume, row_interp, entry)))
    far = lax.ppermute(own, "view", [(i, i ^ CORES) for i in range(views)])
    hi, lo, maps_hi, maps_lo, entry_own = pl.pallas_call(
        functools.partial(prepare_kernel, order, planes),
        out_shape=[
            jax.ShapeDtypeStruct((planes * lateral, span), jnp.bfloat16),
            jax.ShapeDtypeStruct((planes * lateral, span), jnp.bfloat16),
            jax.ShapeDtypeStruct((rows, rows), jnp.bfloat16),
            jax.ShapeDtypeStruct((rows, rows), jnp.bfloat16),
            jax.ShapeDtypeStruct((per, rows), jnp.int32),
        ],
        in_specs=[smem()] * 2 + [vmem()] * 3,
        out_specs=[vmem()] * 5,
        scratch_shapes=[pltpu.VMEM((rows, rows), jnp.float32), pltpu.VMEM((rows, rows), jnp.float32)],
        compiler_params=small(),
        cost_estimate=pl.CostEstimate(flops=2_000_000_000, bytes_accessed=4_000_000, transcendentals=0),
        name="prepare",
    )(view_at, depth_at, vol, row, entry_all)
    hi_swapped, lo_swapped = pl.pallas_call(
        halve_kernel,
        out_shape=[jax.ShapeDtypeStruct((planes * lateral, span), jnp.bfloat16)] * 2,
        in_specs=[vmem()],
        out_specs=[vmem()] * 2,
        compiler_params=small(),
        name="halve",
    )(slab)
    blocks = []
    for flip, packed in enumerate((own, far)):
        blocks = [
            pl.pallas_call(
                functools.partial(send_kernel, order, depth, planes, flip),
                out_shape=jax.ShapeDtypeStruct((len(order) * block_rows, LANES), jnp.float32),
                in_specs=[smem()] + [vmem()] * (6 + len(blocks)),
                out_specs=vmem(),
                input_output_aliases={7: 0} if blocks else {},
                compiler_params=small(),
                cost_estimate=pl.CostEstimate(flops=1_000_000_000, bytes_accessed=2_000_000, transcendentals=0),
            )(view_at, hi, lo, hi_swapped, lo_swapped, coef, packed, *blocks)
        ]
    blocks = blocks[0]
    blocks = blocks.reshape(len(order), block_rows, 1, LANES)
    recv = lax.all_to_all(blocks, ("view", "depth"), split_axis=0, concat_axis=0, tiled=True, axis_index_groups=groups)
    recv = recv.reshape(len(order) * block_rows, LANES)
    image = pl.pallas_call(
        functools.partial(render_kernel, step_length, CORES * planes, order, turn),
        out_shape=jax.ShapeDtypeStruct((depth, SUB, LANES), jnp.float32),
        in_specs=[vmem()] * 4,
        out_specs=vmem(),
        compiler_params=small(),
        name="render",
    )(recv, maps_hi, maps_lo, entry_own)
    turned = lax.all_to_all(image, "depth", split_axis=0, concat_axis=0, tiled=True, axis_index_groups=[turn])
    return pl.pallas_call(
        functools.partial(unpack_kernel, per, turn),
        out_shape=jax.ShapeDtypeStruct((1, 3, rows // depth, lateral), jnp.float32),
        in_specs=[vmem()],
        out_specs=vmem(),
        compiler_params=small(),
        name="unpack",
    )(turned)


def with_arrays(volume, step_weights, row_interp, col_interp, tf_table, materials, entry):
    all_steps = lax.all_gather(step_weights, "view", axis=0, tiled=True)
    all_cols = lax.all_gather(col_interp, "view", axis=0, tiled=True)
    views, steps, edge = all_steps.shape
    depth = lax.axis_size("depth")
    planes, lateral, _ = volume.shape
    devices = views * depth
    per = lateral // depth
    rows = devices * planes
    tiles_z, tiles_y = materials.shape[:2]
    step_length = 2.0 / (steps * depth)
    cells = volume.reshape(planes, tiles_y, edge, depth, edge)
    first = jnp.einsum("pujbi,vsi->vpujbs", cells, all_steps, precision=HIGHEST)
    second = jnp.einsum("vpujbs,vcj->vpucbs", first, all_cols, precision=HIGHEST)
    second = second.reshape(views, planes, depth, per, depth, steps).transpose(0, 2, 1, 3, 4, 5)
    second = second.reshape(devices, planes * per * depth * steps)
    own = tf_table[materials[:, :, 0]].transpose(1, 0, 2).reshape(tiles_y, tiles_z * COEF)
    own = jnp.tile(jnp.repeat(own, edge // per, axis=0), (views, 1))
    payload = jnp.concatenate([second, own], axis=1)
    payload = jnp.pad(payload, ((0, 0), (0, -payload.shape[1] % LANES)))
    payload = payload.reshape(devices, -1, 1, LANES)
    recv = lax.all_to_all(payload, ("view", "depth"), split_axis=0, concat_axis=0, tiled=True)
    recv = recv.reshape(devices, -1)
    size = second.shape[1]
    coef = recv[:depth, size : size + tiles_z * COEF].reshape(depth, tiles_z, COEF)
    coef = jnp.repeat(coef.transpose(2, 1, 0), edge, axis=1)[:, :, None, :, None]
    third = recv[:, :size].reshape(tiles_z, edge, per, depth, steps)
    third = jnp.einsum("tkcbs,rk->trcbs", third, row_interp[0], precision=HIGHEST)
    samples = third.reshape(rows, per, depth, steps)
    entry_own = lax.dynamic_slice_in_dim(entry[0], lax.axis_index("depth") * per, per, 1)
    live = (entry_own[:, :, None] <= jnp.arange(depth)).astype(jnp.float32)
    tau = step_length * live[..., None] * jax.nn.softplus(coef[6] * samples + coef[7])
    flat = tau.reshape(rows, per, depth * steps)
    earlier = (jnp.cumsum(flat, axis=2) - flat).reshape(tau.shape)
    weights = jnp.exp(-earlier) * (1.0 - jnp.exp(-tau))
    emission = jax.nn.softplus(coef[0:3] * samples + coef[3:6])
    image = jnp.sum(weights * emission, axis=(3, 4))
    turned = lax.all_to_all(image, "depth", split_axis=1, concat_axis=2, tiled=True)
    return turned[None]


def shards(volume, step_weights, row_interp, col_interp, tf_table, materials, entry):
    views = lax.axis_size("view")
    depth = lax.axis_size("depth")
    planes, lateral, span = volume.shape
    steps, edge = step_weights.shape[1:]
    rows = views * depth * planes
    fits = (
        depth == SUB
        and steps == SUB
        and edge == LANES // 2
        and lateral == LANES
        and rows == LANES
        and views == 2 * CORES
        and span == depth * edge
    )
    run = with_kernels if fits else with_arrays
    return run(volume, step_weights, row_interp, col_interp, tf_table, materials, entry)


def solution(mesh):
    placed = (
        P(("view", "depth"), None, None),
        P("view", None, None),
        P("view", None, None),
        P("view", None, None),
        P(),
        P(None, None, "depth"),
        P("view", None, None),
    )
    return jax.shard_map(
        shards,
        mesh=mesh,
        in_specs=placed,
        out_specs=P("view", None, "depth", None),
        check_vma=False,
    )
```

```python
import functools

import jax
import jax.numpy as jnp
from jax import lax
from jax.experimental import pallas as pl
from jax.experimental.pallas import tpu as pltpu
from jax.sharding import PartitionSpec as P


LANES = 128
SUB = 8
COEF = 8
CORES = 2
HIGHEST = lax.Precision.HIGHEST
NT = (((1,), (1,)), ((), ()))
NN = (((1,), (0,)), ((), ()))


def split(x):
    hi = x.astype(jnp.bfloat16)
    return hi, (x - hi.astype(jnp.float32)).astype(jnp.bfloat16)


LOG2E = 1.4426950408889634


def softplus(v):
    e = jnp.exp2(jnp.abs(v) * -LOG2E)
    return jnp.maximum(v, 0.0) + jnp.where(e < 2.0**-12, e, jnp.log(1.0 + e))


def fetch_kernel(
    steps_hbm, cols_hbm, classes_hbm, table_hbm, vol_hbm, row_hbm, entry_hbm,
    packed_ref, vol_ref, row_ref, entry_ref, coef_ref,
    steps_ref, cols_ref, classes_ref, table_ref, sems,
):
    pieces = [
        (cols_hbm, cols_ref), (steps_hbm, steps_ref), (classes_hbm, classes_ref), (table_hbm, table_ref),
        (row_hbm, row_ref), (entry_hbm, entry_ref),
    ]
    pieces += [(vol_hbm.at[p], vol_ref.at[p]) for p in range(vol_ref.shape[0])]
    copies = [pltpu.make_async_copy(*piece, sems.at[n]) for n, piece in enumerate(pieces)]
    for copy in copies:
        copy.start()
    for copy in copies[:4]:
        copy.wait()
    edge = cols_ref.shape[1]
    packed_ref[0, : edge // 2] = jnp.concatenate([cols_ref[0, : edge // 2], cols_ref[0, edge // 2 :]], axis=1)
    packed_ref[0, edge // 2 :] = jnp.concatenate([steps_ref[0], steps_ref[0]], axis=1)
    lane = lax.broadcasted_iota(jnp.int32, (1, LANES), 1)
    for u in range(classes_ref.shape[2]):
        row = jnp.zeros((1, LANES), jnp.float32)
        for t in range(classes_ref.shape[0]):
            for ch in range(COEF):
                row = jnp.where(lane == t * COEF + ch, table_ref[classes_ref[t, 0, u], ch], row)
        coef_ref[u : u + 1] = row
    for copy in copies[4:]:
        copy.wait()


def prepare_kernel(
    order, planes, view_ref, depth_ref, vol_ref, row_ref, entry_ref,
    hi_ref, lo_ref, maps_hi_ref, maps_lo_ref, entry_own_ref,
    turned_ref, moved_ref,
):
    per = entry_own_ref.shape[0]
    turned = row_ref[0].T
    zero = jnp.zeros_like(turned)
    tiles_z = turned_ref.shape[0] // turned.shape[0]
    turned_ref[...] = jnp.concatenate(
        [jnp.concatenate([turned if i == t else zero for i in range(tiles_z)], axis=1) for t in range(tiles_z)],
        axis=0,
    )
    core = view_ref[0] % CORES
    depth = entry_ref.shape[2] // per
    for swapped in range(CORES):
        slab = (core ^ swapped) * depth * planes
        for p in range(planes):
            for n, (chip, d) in enumerate(order):
                to = (swapped * planes + p) * len(order) + n
                at = slab + (chip * CORES * depth + d) * planes + p
                moved_ref[to : to + 1] = turned_ref[pl.ds(at, 1), :]
    maps_hi_ref[...], maps_lo_ref[...] = split(moved_ref[...])
    turned = entry_ref[0].astype(jnp.float32).T
    own = jnp.zeros((per, turned.shape[1]), jnp.float32)
    for d in range(depth):
        own = jnp.where(depth_ref[0] == d, turned[d * per : (d + 1) * per], own)
    entry_own_ref[...] = own.astype(jnp.int32)
    halve_kernel(vol_ref, hi_ref, lo_ref)


def halve_kernel(vol_ref, hi_ref, lo_ref):
    lateral = vol_ref.shape[1]
    for p in range(vol_ref.shape[0]):
        at = slice(p * lateral, (p + 1) * lateral)
        hi_ref[at], lo_ref[at] = split(vol_ref[p])


def send_kernel(order, depth, planes, flip, view_ref, hi_ref, lo_ref, hi_swapped_ref, lo_swapped_ref, coef_ref, map_ref, *refs):
    out_ref = refs[-1]
    edge = map_ref.shape[2] // 2
    lateral, span = hi_ref.shape[0] // planes, hi_ref.shape[1]
    bricks = span // edge
    per = lateral // depth
    block_rows = CORES * planes * SUB + 1
    chip = (view_ref[0] // CORES) ^ flip
    starts = []
    for d in range(depth):
        row = order.index((0, d)) * block_rows
        for x in range(1, len(order) // depth):
            row = jnp.where(chip == x, order.index((x, d)) * block_rows, row)
        starts.append(row)

    weights = map_ref[0, edge // 2 :]
    tiled = jnp.concatenate([weights] * (span // LANES), axis=1)
    lane = lax.broadcasted_iota(jnp.int32, (bricks, span), 1)
    brick = lax.broadcasted_iota(jnp.int32, (bricks, span), 0)
    own = lane // edge == brick
    ray = jnp.where(own[None], tiled[:, None, :], 0.0).reshape(weights.shape[0] * bricks, span)
    ray_hi, ray_lo = split(ray)
    ray_hi = jnp.concatenate([ray_hi, ray_hi], axis=0)
    ray_both = jnp.concatenate([ray_hi, ray_lo, ray_lo], axis=0)

    half = lax.broadcasted_iota(jnp.int32, (SUB, LANES), 1) < edge
    left = lax.broadcasted_iota(jnp.int32, (edge // 2, LANES), 1) < edge
    c = map_ref[0, : edge // 2]
    turned = pltpu.roll(c, edge, 1)
    rows = [jnp.where(left, c, 0.0), jnp.where(left, turned, 0.0)]
    rows += [jnp.where(left, 0.0, turned), jnp.where(left, 0.0, c)]
    maps_hi, maps_lo = split(jnp.concatenate(rows, axis=0))
    maps = jnp.concatenate([maps_hi, maps_lo], axis=1)
    for swapped, (high_ref, low_ref) in enumerate(((hi_ref, lo_ref), (hi_swapped_ref, lo_swapped_ref))):
        both = lax.dot_general(high_ref[...], ray_both, NT, preferred_element_type=jnp.float32)
        first = both[:, :LANES] + (
            both[:, LANES:] + lax.dot_general(low_ref[...], ray_hi, NT, preferred_element_type=jnp.float32)
        )
        first_hi, first_lo = split(first)
        for couple in range(planes // 2):
            at = [slice((2 * couple + i) * lateral, (2 * couple + i + 1) * lateral) for i in range(2)]
            high = jnp.concatenate([first_hi[i] for i in at], axis=1)
            low = jnp.concatenate([first_lo[i] for i in at], axis=1)
            second = lax.dot_general(
                maps, jnp.concatenate([high, high], axis=0), NN, preferred_element_type=jnp.float32
            ) + lax.dot_general(maps_hi, low, NN, preferred_element_type=jnp.float32)
            for i in range(2):
                plane = swapped * planes + 2 * couple + i
                for d in range(depth):
                    base = d * per
                    a = second[base : base + SUB, i * LANES : (i + 1) * LANES]
                    b = second[base + SUB : base + 2 * SUB, i * LANES : (i + 1) * LANES]
                    out_ref[pl.ds(starts[d] + plane * SUB, SUB), :] = jnp.where(half, a, b)
    for d in range(depth):
        u = d * per // edge
        out_ref[pl.ds(starts[d] + block_rows - 1, 1), :] = coef_ref[u : u + 1]


def render_kernel(step_length, planes, order, turn, recv_ref, maps_hi_ref, maps_lo_ref, entry_ref, out_ref):
    block_rows = planes * SUB + 1
    sources = len(order)
    columns, rows = entry_ref.shape
    bricks = steps = SUB
    maps_hi = maps_hi_ref[...]
    maps = jnp.concatenate([maps_hi, maps_hi], axis=0)
    maps_lo = maps_lo_ref[...]

    ends = [(order.index((0, b)) + 1) * block_rows for b in range(bricks)]
    packed = jnp.concatenate([recv_ref[end - 1 : end] for end in ends], axis=0)
    lane = lax.broadcasted_iota(jnp.int32, (bricks, rows), 1)
    upper = lane >= rows // 2
    coef = []
    for ch in range(COEF):
        low = jnp.broadcast_to(packed[:, ch : ch + 1], (bricks, rows))
        high = jnp.broadcast_to(packed[:, COEF + ch : COEF + ch + 1], (bricks, rows))
        coef.append(jnp.where(upper, high, low))
    brick = lax.broadcasted_iota(jnp.int32, (bricks, rows), 0)

    shown = [[None] * columns for _ in range(3)]
    for x in range(SUB):
        cells = jnp.concatenate(
            [recv_ref[pl.ds(p * SUB + x, sources, stride=block_rows), :] for p in range(planes)], axis=0
        )
        high, low = split(cells.T)
        samples = lax.dot_general(
            jnp.concatenate([high, low], axis=1), maps, NN, preferred_element_type=jnp.float32
        ) + lax.dot_general(high, maps_lo, NN, preferred_element_type=jnp.float32)
        for m in range(2):
            c = m * SUB + x
            live = jnp.where(entry_ref[c : c + 1, :] <= brick, -step_length * LOG2E, 0.0)
            total = jnp.zeros((bricks, rows), jnp.float32)
            before = jnp.ones((bricks, rows), jnp.float32)
            colours = [jnp.zeros((bricks, rows), jnp.float32) for _ in range(3)]
            for s in range(steps):
                at = (m * steps + s) * bricks
                v = samples[at : at + bricks]
                total = total + live * softplus(coef[6] * v + coef[7])
                after = jnp.exp2(total)
                weight = before - after
                before = after
                for ch in range(3):
                    colours[ch] = colours[ch] + weight * softplus(coef[ch] * v + coef[3 + ch])
            front = total
            for shift in (1, 2, 4):
                front = front + jnp.where(brick >= shift, pltpu.roll(front, shift, 0), 0.0)
            reach = jnp.exp2(front - total)
            for ch in range(3):
                shown[ch][c] = jnp.sum(reach * colours[ch], axis=0, keepdims=True)
    blank = jnp.zeros((LANES // 2 - 3 * columns, rows), jnp.float32)
    image = jnp.concatenate([r for ch in shown for r in ch] + [blank], axis=0)
    image = jnp.concatenate([image, image], axis=0).T
    left = lax.broadcasted_iota(jnp.int32, (SUB, LANES), 1) < LANES // 2
    for n, d in enumerate(turn):
        at = d * 2 * SUB
        out_ref[n] = jnp.where(left, image[at : at + SUB], image[at + SUB : at + 2 * SUB])


def unpack_kernel(columns, turn, recv_ref, out_ref):
    owner = lax.broadcasted_iota(jnp.int32, (SUB, LANES), 1) // columns
    for ch in range(3):
        for h in range(2):
            out = jnp.zeros((SUB, LANES), jnp.float32)
            for n, s in enumerate(turn):
                moved = pltpu.roll(recv_ref[n], ((s - ch) * columns - h * (LANES // 2)) % LANES, 1)
                out = jnp.where(owner == s, moved, out)
            out_ref[0, ch, h * SUB : (h + 1) * SUB] = out


def small():
    return pltpu.CompilerParams(vmem_limit_bytes=16 * 1024 * 1024)


def orders(views, depth):
    chips = views // CORES
    order = [(x, z * 2 + y) for y in range(2) for x in range(chips) for z in range(depth // 2)]
    first = order.index((chips - 1, depth // 2 + 1))
    turn = depth // 2 + 1
    return order[first:] + order[:first], list(range(turn, depth)) + list(range(turn))


def vmem():
    return pl.BlockSpec(memory_space=pltpu.VMEM)


def hbm():
    return pl.BlockSpec(memory_space=pltpu.HBM)


def in_hbm(x):
    return pltpu.with_memory_space_constraint(x, pltpu.HBM)


def smem():
    return pl.BlockSpec(memory_space=pltpu.SMEM)


def with_kernels(volume, step_weights, row_interp, col_interp, tf_table, materials, entry):
    views = lax.axis_size("view")
    steps, edge = step_weights.shape[1:]
    depth = lax.axis_size("depth")
    planes, lateral, span = volume.shape
    devices = views * depth
    per = lateral // depth
    rows = devices * planes
    step_length = 2.0 / (steps * depth)
    tiles_y = lateral // edge
    block_rows = CORES * planes * SUB + 1
    order, turn = orders(views, depth)
    groups = [[(x * CORES + core) * depth + d for x, d in order] for core in range(CORES)]
    depth_at = lax.axis_index("depth").reshape(1)
    view_at = lax.axis_index("view").reshape(1)
    slab = lax.ppermute(volume, "view", [(i, i ^ 1) for i in range(views)])
    own, vol, row, entry_all, coef = pl.pallas_call(
        fetch_kernel,
        out_shape=[
            jax.ShapeDtypeStruct((1, edge // 2 + steps, 2 * edge), jnp.float32),
            jax.ShapeDtypeStruct(volume.shape, volume.dtype),
            jax.ShapeDtypeStruct(row_interp.shape, row_interp.dtype),
            jax.ShapeDtypeStruct(entry.shape, entry.dtype),
            jax.ShapeDtypeStruct((tiles_y, LANES), jnp.float32),
        ],
        in_specs=[hbm()] * 7,
        out_specs=[vmem()] * 5,
        scratch_shapes=[
            pltpu.VMEM(step_weights.shape, jnp.float32),
            pltpu.VMEM(col_interp.shape, jnp.float32),
            pltpu.SMEM((materials.shape[0], 1, tiles_y), jnp.int32),
            pltpu.SMEM(tf_table.shape, jnp.float32),
            pltpu.SemaphoreType.DMA((planes + 6,)),
        ],
        compiler_params=small(),
        name="fetch",
    )(*map(in_hbm, (step_weights, col_interp, materials.transpose(0, 2, 1), tf_table, volume, row_interp, entry)))
    far = lax.ppermute(own, "view", [(i, i ^ CORES) for i in range(views)])
    hi, lo, maps_hi, maps_lo, entry_own = pl.pallas_call(
        functools.partial(prepare_kernel, order, planes),
        out_shape=[
            jax.ShapeDtypeStruct((planes * lateral, span), jnp.bfloat16),
            jax.ShapeDtypeStruct((planes * lateral, span), jnp.bfloat16),
            jax.ShapeDtypeStruct((rows, rows), jnp.bfloat16),
            jax.ShapeDtypeStruct((rows, rows), jnp.bfloat16),
            jax.ShapeDtypeStruct((per, rows), jnp.int32),
        ],
        in_specs=[smem()] * 2 + [vmem()] * 3,
        out_specs=[vmem()] * 5,
        scratch_shapes=[pltpu.VMEM((rows, rows), jnp.float32), pltpu.VMEM((rows, rows), jnp.float32)],
        compiler_params=small(),
        cost_estimate=pl.CostEstimate(flops=2_000_000_000, bytes_accessed=4_000_000, transcendentals=0),
        name="prepare",
    )(view_at, depth_at, vol, row, entry_all)
    hi_swapped, lo_swapped = pl.pallas_call(
        halve_kernel,
        out_shape=[jax.ShapeDtypeStruct((planes * lateral, span), jnp.bfloat16)] * 2,
        in_specs=[vmem()],
        out_specs=[vmem()] * 2,
        compiler_params=small(),
        name="halve",
    )(slab)
    blocks = []
    for flip, packed in enumerate((own, far)):
        blocks = [
            pl.pallas_call(
                functools.partial(send_kernel, order, depth, planes, flip),
                out_shape=jax.ShapeDtypeStruct((len(order) * block_rows, LANES), jnp.float32),
                in_specs=[smem()] + [vmem()] * (6 + len(blocks)),
                out_specs=vmem(),
                input_output_aliases={7: 0} if blocks else {},
                compiler_params=small(),
                cost_estimate=pl.CostEstimate(flops=1_000_000_000, bytes_accessed=2_000_000, transcendentals=0),
            )(view_at, hi, lo, hi_swapped, lo_swapped, coef, packed, *blocks)
        ]
    blocks = blocks[0]
    blocks = blocks.reshape(len(order), block_rows, 1, LANES)
    recv = lax.all_to_all(blocks, ("view", "depth"), split_axis=0, concat_axis=0, tiled=True, axis_index_groups=groups)
    recv = recv.reshape(len(order) * block_rows, LANES)
    image = pl.pallas_call(
        functools.partial(render_kernel, step_length, CORES * planes, order, turn),
        out_shape=jax.ShapeDtypeStruct((depth, SUB, LANES), jnp.float32),
        in_specs=[vmem()] * 4,
        out_specs=vmem(),
        compiler_params=small(),
        name="render",
    )(recv, maps_hi, maps_lo, entry_own)
    turned = lax.all_to_all(image, "depth", split_axis=0, concat_axis=0, tiled=True, axis_index_groups=[turn])
    return pl.pallas_call(
        functools.partial(unpack_kernel, per, turn),
        out_shape=jax.ShapeDtypeStruct((1, 3, rows // depth, lateral), jnp.float32),
        in_specs=[vmem()],
        out_specs=vmem(),
        compiler_params=small(),
        name="unpack",
    )(turned)


def with_arrays(volume, step_weights, row_interp, col_interp, tf_table, materials, entry):
    all_steps = lax.all_gather(step_weights, "view", axis=0, tiled=True)
    all_cols = lax.all_gather(col_interp, "view", axis=0, tiled=True)
    views, steps, edge = all_steps.shape
    depth = lax.axis_size("depth")
    planes, lateral, _ = volume.shape
    devices = views * depth
    per = lateral // depth
    rows = devices * planes
    tiles_z, tiles_y = materials.shape[:2]
    step_length = 2.0 / (steps * depth)
    cells = volume.reshape(planes, tiles_y, edge, depth, edge)
    first = jnp.einsum("pujbi,vsi->vpujbs", cells, all_steps, precision=HIGHEST)
    second = jnp.einsum("vpujbs,vcj->vpucbs", first, all_cols, precision=HIGHEST)
    second = second.reshape(views, planes, depth, per, depth, steps).transpose(0, 2, 1, 3, 4, 5)
    second = second.reshape(devices, planes * per * depth * steps)
    own = tf_table[materials[:, :, 0]].transpose(1, 0, 2).reshape(tiles_y, tiles_z * COEF)
    own = jnp.tile(jnp.repeat(own, edge // per, axis=0), (views, 1))
    payload = jnp.concatenate([second, own], axis=1)
    payload = jnp.pad(payload, ((0, 0), (0, -payload.shape[1] % LANES)))
    payload = payload.reshape(devices, -1, 1, LANES)
    recv = lax.all_to_all(payload, ("view", "depth"), split_axis=0, concat_axis=0, tiled=True)
    recv = recv.reshape(devices, -1)
    size = second.shape[1]
    coef = recv[:depth, size : size + tiles_z * COEF].reshape(depth, tiles_z, COEF)
    coef = jnp.repeat(coef.transpose(2, 1, 0), edge, axis=1)[:, :, None, :, None]
    third = recv[:, :size].reshape(tiles_z, edge, per, depth, steps)
    third = jnp.einsum("tkcbs,rk->trcbs", third, row_interp[0], precision=HIGHEST)
    samples = third.reshape(rows, per, depth, steps)
    entry_own = lax.dynamic_slice_in_dim(entry[0], lax.axis_index("depth") * per, per, 1)
    live = (entry_own[:, :, None] <= jnp.arange(depth)).astype(jnp.float32)
    tau = step_length * live[..., None] * jax.nn.softplus(coef[6] * samples + coef[7])
    flat = tau.reshape(rows, per, depth * steps)
    earlier = (jnp.cumsum(flat, axis=2) - flat).reshape(tau.shape)
    weights = jnp.exp(-earlier) * (1.0 - jnp.exp(-tau))
    emission = jax.nn.softplus(coef[0:3] * samples + coef[3:6])
    image = jnp.sum(weights * emission, axis=(3, 4))
    turned = lax.all_to_all(image, "depth", split_axis=1, concat_axis=2, tiled=True)
    return turned[None]


def shards(volume, step_weights, row_interp, col_interp, tf_table, materials, entry):
    views = lax.axis_size("view")
    depth = lax.axis_size("depth")
    planes, lateral, span = volume.shape
    steps, edge = step_weights.shape[1:]
    rows = views * depth * planes
    fits = (
        depth == SUB
        and steps == SUB
        and edge == LANES // 2
        and lateral == LANES
        and rows == LANES
        and views == 2 * CORES
        and span == depth * edge
    )
    run = with_kernels if fits else with_arrays
    return run(volume, step_weights, row_interp, col_interp, tf_table, materials, entry)


def solution(mesh):
    placed = (
        P(("view", "depth"), None, None),
        P("view", None, None),
        P("view", None, None),
        P("view", None, None),
        P(),
        P(None, None, "depth"),
        P("view", None, None),
    )
    return jax.shard_map(
        shards,
        mesh=mesh,
        in_specs=placed,
        out_specs=P("view", None, "depth", None),
        check_vma=False,
    )
```

```python
import functools

import jax
import jax.numpy as jnp
from jax import lax
from jax.experimental import pallas as pl
from jax.experimental.pallas import tpu as pltpu
from jax.sharding import PartitionSpec as P


LANES = 128
SUB = 8
COEF = 8
CORES = 2
HIGHEST = lax.Precision.HIGHEST
NT = (((1,), (1,)), ((), ()))
NN = (((1,), (0,)), ((), ()))


def split(x):
    hi = x.astype(jnp.bfloat16)
    return hi, (x - hi.astype(jnp.float32)).astype(jnp.bfloat16)


LOG2E = 1.4426950408889634


def softplus(v):
    e = jnp.exp2(jnp.abs(v) * -LOG2E)
    return jnp.maximum(v, 0.0) + jnp.where(e < 2.0**-12, e, jnp.log(1.0 + e))


def fetch_kernel(
    steps_hbm, cols_hbm, classes_hbm, table_hbm, row_hbm, entry_hbm,
    packed_ref, row_ref, entry_ref, coef_ref,
    steps_ref, cols_ref, classes_ref, table_ref, sems,
):
    pieces = [
        (cols_hbm, cols_ref), (steps_hbm, steps_ref), (classes_hbm, classes_ref), (table_hbm, table_ref),
        (row_hbm, row_ref), (entry_hbm, entry_ref),
    ]
    copies = [pltpu.make_async_copy(*piece, sems.at[n]) for n, piece in enumerate(pieces)]
    for copy in copies:
        copy.start()
    for copy in copies[:4]:
        copy.wait()
    edge = cols_ref.shape[1]
    packed_ref[0, : edge // 2] = jnp.concatenate([cols_ref[0, : edge // 2], cols_ref[0, edge // 2 :]], axis=1)
    packed_ref[0, edge // 2 :] = jnp.concatenate([steps_ref[0], steps_ref[0]], axis=1)
    lane = lax.broadcasted_iota(jnp.int32, (1, LANES), 1)
    for u in range(classes_ref.shape[2]):
        row = jnp.zeros((1, LANES), jnp.float32)
        for t in range(classes_ref.shape[0]):
            for ch in range(COEF):
                row = jnp.where(lane == t * COEF + ch, table_ref[classes_ref[t, 0, u], ch], row)
        coef_ref[u : u + 1] = row
    for copy in copies[4:]:
        copy.wait()


def prepare_kernel(
    order, planes, view_ref, depth_ref, vol_ref, row_ref, entry_ref,
    hi_ref, lo_ref, maps_hi_ref, maps_lo_ref, entry_own_ref,
    turned_ref, moved_ref,
):
    per = entry_own_ref.shape[0]
    turned = row_ref[0].T
    zero = jnp.zeros_like(turned)
    tiles_z = turned_ref.shape[0] // turned.shape[0]
    turned_ref[...] = jnp.concatenate(
        [jnp.concatenate([turned if i == t else zero for i in range(tiles_z)], axis=1) for t in range(tiles_z)],
        axis=0,
    )
    core = view_ref[0] % CORES
    depth = entry_ref.shape[2] // per
    for swapped in range(CORES):
        slab = (core ^ swapped) * depth * planes
        for p in range(planes):
            for n, (chip, d) in enumerate(order):
                to = (swapped * planes + p) * len(order) + n
                at = slab + (chip * CORES * depth + d) * planes + p
                moved_ref[to : to + 1] = turned_ref[pl.ds(at, 1), :]
    maps_hi_ref[...], maps_lo_ref[...] = split(moved_ref[...])
    turned = entry_ref[0].astype(jnp.float32).T
    own = jnp.zeros((per, turned.shape[1]), jnp.float32)
    for d in range(depth):
        own = jnp.where(depth_ref[0] == d, turned[d * per : (d + 1) * per], own)
    entry_own_ref[...] = own.astype(jnp.int32)
    halve_kernel(vol_ref, hi_ref, lo_ref)


def halve_kernel(vol_ref, hi_ref, lo_ref):
    lateral = vol_ref.shape[1]
    for p in range(vol_ref.shape[0]):
        at = slice(p * lateral, (p + 1) * lateral)
        hi_ref[at], lo_ref[at] = split(vol_ref[p])


def send_kernel(order, depth, planes, flip, view_ref, hi_ref, lo_ref, hi_swapped_ref, lo_swapped_ref, coef_ref, map_ref, *refs):
    out_ref = refs[-1]
    edge = map_ref.shape[2] // 2
    lateral, span = hi_ref.shape[0] // planes, hi_ref.shape[1]
    bricks = span // edge
    per = lateral // depth
    block_rows = CORES * planes * SUB + 1
    chip = (view_ref[0] // CORES) ^ flip
    starts = []
    for d in range(depth):
        row = order.index((0, d)) * block_rows
        for x in range(1, len(order) // depth):
            row = jnp.where(chip == x, order.index((x, d)) * block_rows, row)
        starts.append(row)

    weights = map_ref[0, edge // 2 :]
    tiled = jnp.concatenate([weights] * (span // LANES), axis=1)
    lane = lax.broadcasted_iota(jnp.int32, (bricks, span), 1)
    brick = lax.broadcasted_iota(jnp.int32, (bricks, span), 0)
    own = lane // edge == brick
    ray = jnp.where(own[None], tiled[:, None, :], 0.0).reshape(weights.shape[0] * bricks, span)
    ray_hi, ray_lo = split(ray)
    ray_hi = jnp.concatenate([ray_hi, ray_hi], axis=0)
    ray_both = jnp.concatenate([ray_hi, ray_lo, ray_lo], axis=0)

    half = lax.broadcasted_iota(jnp.int32, (SUB, LANES), 1) < edge
    left = lax.broadcasted_iota(jnp.int32, (edge // 2, LANES), 1) < edge
    c = map_ref[0, : edge // 2]
    turned = pltpu.roll(c, edge, 1)
    rows = [jnp.where(left, c, 0.0), jnp.where(left, turned, 0.0)]
    rows += [jnp.where(left, 0.0, turned), jnp.where(left, 0.0, c)]
    maps_hi, maps_lo = split(jnp.concatenate(rows, axis=0))
    maps = jnp.concatenate([maps_hi, maps_lo], axis=1)
    for swapped, (high_ref, low_ref) in enumerate(((hi_ref, lo_ref), (hi_swapped_ref, lo_swapped_ref))):
        both = lax.dot_general(high_ref[...], ray_both, NT, preferred_element_type=jnp.float32)
        first = both[:, :LANES] + (
            both[:, LANES:] + lax.dot_general(low_ref[...], ray_hi, NT, preferred_element_type=jnp.float32)
        )
        first_hi, first_lo = split(first)
        for couple in range(planes // 2):
            at = [slice((2 * couple + i) * lateral, (2 * couple + i + 1) * lateral) for i in range(2)]
            high = jnp.concatenate([first_hi[i] for i in at], axis=1)
            low = jnp.concatenate([first_lo[i] for i in at], axis=1)
            second = lax.dot_general(
                maps, jnp.concatenate([high, high], axis=0), NN, preferred_element_type=jnp.float32
            ) + lax.dot_general(maps_hi, low, NN, preferred_element_type=jnp.float32)
            for i in range(2):
                plane = swapped * planes + 2 * couple + i
                for d in range(depth):
                    base = d * per
                    a = second[base : base + SUB, i * LANES : (i + 1) * LANES]
                    b = second[base + SUB : base + 2 * SUB, i * LANES : (i + 1) * LANES]
                    out_ref[pl.ds(starts[d] + plane * SUB, SUB), :] = jnp.where(half, a, b)
    for d in range(depth):
        u = d * per // edge
        out_ref[pl.ds(starts[d] + block_rows - 1, 1), :] = coef_ref[u : u + 1]


def render_kernel(step_length, planes, order, turn, recv_ref, maps_hi_ref, maps_lo_ref, entry_ref, out_ref):
    block_rows = planes * SUB + 1
    sources = len(order)
    columns, rows = entry_ref.shape
    bricks = steps = SUB
    maps_hi = maps_hi_ref[...]
    maps = jnp.concatenate([maps_hi, maps_hi], axis=0)
    maps_lo = maps_lo_ref[...]

    ends = [(order.index((0, b)) + 1) * block_rows for b in range(bricks)]
    packed = jnp.concatenate([recv_ref[end - 1 : end] for end in ends], axis=0)
    lane = lax.broadcasted_iota(jnp.int32, (bricks, rows), 1)
    upper = lane >= rows // 2
    coef = []
    for ch in range(COEF):
        low = jnp.broadcast_to(packed[:, ch : ch + 1], (bricks, rows))
        high = jnp.broadcast_to(packed[:, COEF + ch : COEF + ch + 1], (bricks, rows))
        coef.append(jnp.where(upper, high, low))
    brick = lax.broadcasted_iota(jnp.int32, (bricks, rows), 0)

    shown = [[None] * columns for _ in range(3)]
    for x in range(SUB):
        cells = jnp.concatenate(
            [recv_ref[pl.ds(p * SUB + x, sources, stride=block_rows), :] for p in range(planes)], axis=0
        )
        high, low = split(cells.T)
        samples = lax.dot_general(
            jnp.concatenate([high, low], axis=1), maps, NN, preferred_element_type=jnp.float32
        ) + lax.dot_general(high, maps_lo, NN, preferred_element_type=jnp.float32)
        for m in range(2):
            c = m * SUB + x
            live = jnp.where(entry_ref[c : c + 1, :] <= brick, -step_length * LOG2E, 0.0)
            total = jnp.zeros((bricks, rows), jnp.float32)
            before = jnp.ones((bricks, rows), jnp.float32)
            colours = [jnp.zeros((bricks, rows), jnp.float32) for _ in range(3)]
            for s in range(steps):
                at = (m * steps + s) * bricks
                v = samples[at : at + bricks]
                total = total + live * softplus(coef[6] * v + coef[7])
                after = jnp.exp2(total)
                weight = before - after
                before = after
                for ch in range(3):
                    colours[ch] = colours[ch] + weight * softplus(coef[ch] * v + coef[3 + ch])
            front = jnp.where(brick >= 1, pltpu.roll(total, 1, 0), 0.0)
            for shift in (1, 2, 4):
                front = front + jnp.where(brick >= shift, pltpu.roll(front, shift, 0), 0.0)
            reach = jnp.exp2(front)
            for ch in range(3):
                shown[ch][c] = jnp.sum(reach * colours[ch], axis=0, keepdims=True)
    blank = jnp.zeros((LANES // 2 - 3 * columns, rows), jnp.float32)
    image = jnp.concatenate([r for ch in shown for r in ch] + [blank], axis=0)
    image = jnp.concatenate([image, image], axis=0).T
    left = lax.broadcasted_iota(jnp.int32, (SUB, LANES), 1) < LANES // 2
    for n, d in enumerate(turn):
        at = d * 2 * SUB
        out_ref[n] = jnp.where(left, image[at : at + SUB], image[at + SUB : at + 2 * SUB])


def unpack_kernel(columns, turn, recv_ref, out_ref):
    owner = lax.broadcasted_iota(jnp.int32, (SUB, LANES), 1) // columns
    for ch in range(3):
        for h in range(2):
            out = jnp.zeros((SUB, LANES), jnp.float32)
            for n, s in enumerate(turn):
                moved = pltpu.roll(recv_ref[n], ((s - ch) * columns - h * (LANES // 2)) % LANES, 1)
                out = jnp.where(owner == s, moved, out)
            out_ref[0, ch, h * SUB : (h + 1) * SUB] = out


def small():
    return pltpu.CompilerParams(vmem_limit_bytes=16 * 1024 * 1024)


def orders(views, depth):
    chips = views // CORES
    order = [(x, z * 2 + y) for y in range(2) for x in range(chips) for z in range(depth // 2)]
    first = order.index((chips - 1, depth // 2 + 1))
    turn = depth // 2 + 1
    return order[first:] + order[:first], list(range(turn, depth)) + list(range(turn))


def vmem():
    return pl.BlockSpec(memory_space=pltpu.VMEM)


def hbm():
    return pl.BlockSpec(memory_space=pltpu.HBM)


def in_hbm(x):
    return pltpu.with_memory_space_constraint(x, pltpu.HBM)


def smem():
    return pl.BlockSpec(memory_space=pltpu.SMEM)


def with_kernels(volume, step_weights, row_interp, col_interp, tf_table, materials, entry):
    views = lax.axis_size("view")
    steps, edge = step_weights.shape[1:]
    depth = lax.axis_size("depth")
    planes, lateral, span = volume.shape
    devices = views * depth
    per = lateral // depth
    rows = devices * planes
    step_length = 2.0 / (steps * depth)
    tiles_y = lateral // edge
    block_rows = CORES * planes * SUB + 1
    order, turn = orders(views, depth)
    groups = [[(x * CORES + core) * depth + d for x, d in order] for core in range(CORES)]
    depth_at = lax.axis_index("depth").reshape(1)
    view_at = lax.axis_index("view").reshape(1)
    slab = lax.ppermute(volume, "view", [(i, i ^ 1) for i in range(views)])
    own, row, entry_all, coef = pl.pallas_call(
        fetch_kernel,
        out_shape=[
            jax.ShapeDtypeStruct((1, edge // 2 + steps, 2 * edge), jnp.float32),
            jax.ShapeDtypeStruct(row_interp.shape, row_interp.dtype),
            jax.ShapeDtypeStruct(entry.shape, entry.dtype),
            jax.ShapeDtypeStruct((tiles_y, LANES), jnp.float32),
        ],
        in_specs=[hbm()] * 6,
        out_specs=[vmem()] * 4,
        scratch_shapes=[
            pltpu.VMEM(step_weights.shape, jnp.float32),
            pltpu.VMEM(col_interp.shape, jnp.float32),
            pltpu.SMEM((materials.shape[0], 1, tiles_y), jnp.int32),
            pltpu.SMEM(tf_table.shape, jnp.float32),
            pltpu.SemaphoreType.DMA((6,)),
        ],
        compiler_params=small(),
        cost_estimate=pl.CostEstimate(flops=4_000_000_000, bytes_accessed=8_000_000, transcendentals=0),
        name="fetch",
    )(*map(in_hbm, (step_weights, col_interp, materials.transpose(0, 2, 1), tf_table, row_interp, entry)))
    far = lax.ppermute(own, "view", [(i, i ^ CORES) for i in range(views)])
    hi, lo, maps_hi, maps_lo, entry_own = pl.pallas_call(
        functools.partial(prepare_kernel, order, planes),
        out_shape=[
            jax.ShapeDtypeStruct((planes * lateral, span), jnp.bfloat16),
            jax.ShapeDtypeStruct((planes * lateral, span), jnp.bfloat16),
            jax.ShapeDtypeStruct((rows, rows), jnp.bfloat16),
            jax.ShapeDtypeStruct((rows, rows), jnp.bfloat16),
            jax.ShapeDtypeStruct((per, rows), jnp.int32),
        ],
        in_specs=[smem()] * 2 + [vmem()] * 3,
        out_specs=[vmem()] * 5,
        scratch_shapes=[pltpu.VMEM((rows, rows), jnp.float32), pltpu.VMEM((rows, rows), jnp.float32)],
        compiler_params=small(),
        cost_estimate=pl.CostEstimate(flops=2_000_000_000, bytes_accessed=4_000_000, transcendentals=0),
        name="prepare",
    )(view_at, depth_at, volume, row, entry_all)
    hi_swapped, lo_swapped = pl.pallas_call(
        halve_kernel,
        out_shape=[jax.ShapeDtypeStruct((planes * lateral, span), jnp.bfloat16)] * 2,
        in_specs=[vmem()],
        out_specs=[vmem()] * 2,
        compiler_params=small(),
        name="halve",
    )(slab)
    blocks = []
    for flip, packed in enumerate((own, far)):
        blocks = [
            pl.pallas_call(
                functools.partial(send_kernel, order, depth, planes, flip),
                out_shape=jax.ShapeDtypeStruct((len(order) * block_rows, LANES), jnp.float32),
                in_specs=[smem()] + [vmem()] * (6 + len(blocks)),
                out_specs=vmem(),
                input_output_aliases={7: 0} if blocks else {},
                compiler_params=small(),
                cost_estimate=pl.CostEstimate(flops=1_000_000_000, bytes_accessed=2_000_000, transcendentals=0),
            )(view_at, hi, lo, hi_swapped, lo_swapped, coef, packed, *blocks)
        ]
    blocks = blocks[0]
    blocks = blocks.reshape(len(order), block_rows, 1, LANES)
    recv = lax.all_to_all(blocks, ("view", "depth"), split_axis=0, concat_axis=0, tiled=True, axis_index_groups=groups)
    recv = recv.reshape(len(order) * block_rows, LANES)
    image = pl.pallas_call(
        functools.partial(render_kernel, step_length, CORES * planes, order, turn),
        out_shape=jax.ShapeDtypeStruct((depth, SUB, LANES), jnp.float32),
        in_specs=[vmem()] * 4,
        out_specs=vmem(),
        compiler_params=small(),
        name="render",
    )(recv, maps_hi, maps_lo, entry_own)
    turned = lax.all_to_all(image, "depth", split_axis=0, concat_axis=0, tiled=True, axis_index_groups=[turn])
    return pl.pallas_call(
        functools.partial(unpack_kernel, per, turn),
        out_shape=jax.ShapeDtypeStruct((1, 3, rows // depth, lateral), jnp.float32),
        in_specs=[vmem()],
        out_specs=vmem(),
        compiler_params=small(),
        name="unpack",
    )(turned)


def with_arrays(volume, step_weights, row_interp, col_interp, tf_table, materials, entry):
    all_steps = lax.all_gather(step_weights, "view", axis=0, tiled=True)
    all_cols = lax.all_gather(col_interp, "view", axis=0, tiled=True)
    views, steps, edge = all_steps.shape
    depth = lax.axis_size("depth")
    planes, lateral, _ = volume.shape
    devices = views * depth
    per = lateral // depth
    rows = devices * planes
    tiles_z, tiles_y = materials.shape[:2]
    step_length = 2.0 / (steps * depth)
    cells = volume.reshape(planes, tiles_y, edge, depth, edge)
    first = jnp.einsum("pujbi,vsi->vpujbs", cells, all_steps, precision=HIGHEST)
    second = jnp.einsum("vpujbs,vcj->vpucbs", first, all_cols, precision=HIGHEST)
    second = second.reshape(views, planes, depth, per, depth, steps).transpose(0, 2, 1, 3, 4, 5)
    second = second.reshape(devices, planes * per * depth * steps)
    own = tf_table[materials[:, :, 0]].transpose(1, 0, 2).reshape(tiles_y, tiles_z * COEF)
    own = jnp.tile(jnp.repeat(own, edge // per, axis=0), (views, 1))
    payload = jnp.concatenate([second, own], axis=1)
    payload = jnp.pad(payload, ((0, 0), (0, -payload.shape[1] % LANES)))
    payload = payload.reshape(devices, -1, 1, LANES)
    recv = lax.all_to_all(payload, ("view", "depth"), split_axis=0, concat_axis=0, tiled=True)
    recv = recv.reshape(devices, -1)
    size = second.shape[1]
    coef = recv[:depth, size : size + tiles_z * COEF].reshape(depth, tiles_z, COEF)
    coef = jnp.repeat(coef.transpose(2, 1, 0), edge, axis=1)[:, :, None, :, None]
    third = recv[:, :size].reshape(tiles_z, edge, per, depth, steps)
    third = jnp.einsum("tkcbs,rk->trcbs", third, row_interp[0], precision=HIGHEST)
    samples = third.reshape(rows, per, depth, steps)
    entry_own = lax.dynamic_slice_in_dim(entry[0], lax.axis_index("depth") * per, per, 1)
    live = (entry_own[:, :, None] <= jnp.arange(depth)).astype(jnp.float32)
    tau = step_length * live[..., None] * jax.nn.softplus(coef[6] * samples + coef[7])
    flat = tau.reshape(rows, per, depth * steps)
    earlier = (jnp.cumsum(flat, axis=2) - flat).reshape(tau.shape)
    weights = jnp.exp(-earlier) * (1.0 - jnp.exp(-tau))
    emission = jax.nn.softplus(coef[0:3] * samples + coef[3:6])
    image = jnp.sum(weights * emission, axis=(3, 4))
    turned = lax.all_to_all(image, "depth", split_axis=1, concat_axis=2, tiled=True)
    return turned[None]


def shards(volume, step_weights, row_interp, col_interp, tf_table, materials, entry):
    views = lax.axis_size("view")
    depth = lax.axis_size("depth")
    planes, lateral, span = volume.shape
    steps, edge = step_weights.shape[1:]
    rows = views * depth * planes
    fits = (
        depth == SUB
        and steps == SUB
        and edge == LANES // 2
        and lateral == LANES
        and rows == LANES
        and views == 2 * CORES
        and span == depth * edge
    )
    run = with_kernels if fits else with_arrays
    return run(volume, step_weights, row_interp, col_interp, tf_table, materials, entry)


def solution(mesh):
    placed = (
        P(("view", "depth"), None, None),
        P("view", None, None),
        P("view", None, None),
        P("view", None, None),
        P(),
        P(None, None, "depth"),
        P("view", None, None),
    )
    return jax.shard_map(
        shards,
        mesh=mesh,
        in_specs=placed,
        out_specs=P("view", None, "depth", None),
        check_vma=False,
    )
```

```python
import functools

import jax
import jax.numpy as jnp
from jax import lax
from jax.experimental import pallas as pl
from jax.experimental.pallas import tpu as pltpu
from jax.sharding import PartitionSpec as P


LANES = 128
SUB = 8
COEF = 8
CORES = 2
HIGHEST = lax.Precision.HIGHEST
NT = (((1,), (1,)), ((), ()))
NN = (((1,), (0,)), ((), ()))


def split(x):
    hi = x.astype(jnp.bfloat16)
    return hi, (x - hi.astype(jnp.float32)).astype(jnp.bfloat16)


LOG2E = 1.4426950408889634


def softplus(v):
    e = jnp.exp2(jnp.abs(v) * -LOG2E)
    return jnp.maximum(v, 0.0) + jnp.where(e < 2.0**-12, e, jnp.log(1.0 + e))


def fetch_kernel(
    steps_hbm, cols_hbm, classes_hbm, table_hbm, row_hbm, entry_hbm,
    packed_ref, row_ref, entry_ref, coef_ref,
    steps_ref, cols_ref, classes_ref, table_ref, sems,
):
    pieces = [
        (cols_hbm, cols_ref), (steps_hbm, steps_ref), (classes_hbm, classes_ref), (table_hbm, table_ref),
        (row_hbm, row_ref), (entry_hbm, entry_ref),
    ]
    copies = [pltpu.make_async_copy(*piece, sems.at[n]) for n, piece in enumerate(pieces)]
    for copy in copies:
        copy.start()
    for copy in copies[:4]:
        copy.wait()
    edge = cols_ref.shape[1]
    packed_ref[0, : edge // 2] = jnp.concatenate([cols_ref[0, : edge // 2], cols_ref[0, edge // 2 :]], axis=1)
    packed_ref[0, edge // 2 :] = jnp.concatenate([steps_ref[0], steps_ref[0]], axis=1)
    lane = lax.broadcasted_iota(jnp.int32, (1, LANES), 1)
    for u in range(classes_ref.shape[2]):
        row = jnp.zeros((1, LANES), jnp.float32)
        for t in range(classes_ref.shape[0]):
            for ch in range(COEF):
                row = jnp.where(lane == t * COEF + ch, table_ref[classes_ref[t, 0, u], ch], row)
        coef_ref[u : u + 1] = row
    for copy in copies[4:]:
        copy.wait()


def prepare_kernel(
    order, planes, view_ref, depth_ref, vol_ref, row_ref, entry_ref,
    hi_ref, lo_ref, maps_hi_ref, maps_lo_ref, entry_own_ref,
    turned_ref, moved_ref,
):
    per = entry_own_ref.shape[0]
    turned = row_ref[0].T
    zero = jnp.zeros_like(turned)
    tiles_z = turned_ref.shape[0] // turned.shape[0]
    turned_ref[...] = jnp.concatenate(
        [jnp.concatenate([turned if i == t else zero for i in range(tiles_z)], axis=1) for t in range(tiles_z)],
        axis=0,
    )
    core = view_ref[0] % CORES
    depth = entry_ref.shape[2] // per
    for swapped in range(CORES):
        slab = (core ^ swapped) * depth * planes
        for p in range(planes):
            for n, (chip, d) in enumerate(order):
                to = (swapped * planes + p) * len(order) + n
                at = slab + (chip * CORES * depth + d) * planes + p
                moved_ref[to : to + 1] = turned_ref[pl.ds(at, 1), :]
    maps_hi_ref[...], maps_lo_ref[...] = split(moved_ref[...])
    turned = entry_ref[0].astype(jnp.float32).T
    own = jnp.zeros((per, turned.shape[1]), jnp.float32)
    for d in range(depth):
        own = jnp.where(depth_ref[0] == d, turned[d * per : (d + 1) * per], own)
    entry_own_ref[...] = own.astype(jnp.int32)
    halve_kernel(vol_ref, hi_ref, lo_ref)


def halve_kernel(vol_ref, hi_ref, lo_ref):
    lateral = vol_ref.shape[1]
    for p in range(vol_ref.shape[0]):
        at = slice(p * lateral, (p + 1) * lateral)
        hi_ref[at], lo_ref[at] = split(vol_ref[p])


def send_kernel(order, depth, planes, flip, view_ref, hi_ref, lo_ref, coef_ref, map_ref, *refs):
    if flip:
        hi_swapped_ref, lo_swapped_ref, _, out_ref = refs
    else:
        slab_ref, out_ref, hi_swapped_ref, lo_swapped_ref = refs
        halve_kernel(slab_ref, hi_swapped_ref, lo_swapped_ref)
    edge = map_ref.shape[2] // 2
    lateral, span = hi_ref.shape[0] // planes, hi_ref.shape[1]
    bricks = span // edge
    per = lateral // depth
    block_rows = CORES * planes * SUB + 1
    chip = (view_ref[0] // CORES) ^ flip
    starts = []
    for d in range(depth):
        row = order.index((0, d)) * block_rows
        for x in range(1, len(order) // depth):
            row = jnp.where(chip == x, order.index((x, d)) * block_rows, row)
        starts.append(row)

    weights = map_ref[0, edge // 2 :]
    tiled = jnp.concatenate([weights] * (span // LANES), axis=1)
    lane = lax.broadcasted_iota(jnp.int32, (bricks, span), 1)
    brick = lax.broadcasted_iota(jnp.int32, (bricks, span), 0)
    own = lane // edge == brick
    ray = jnp.where(own[None], tiled[:, None, :], 0.0).reshape(weights.shape[0] * bricks, span)
    ray_hi, ray_lo = split(ray)
    ray_hi = jnp.concatenate([ray_hi, ray_hi], axis=0)
    ray_both = jnp.concatenate([ray_hi, ray_lo, ray_lo], axis=0)

    half = lax.broadcasted_iota(jnp.int32, (SUB, LANES), 1) < edge
    left = lax.broadcasted_iota(jnp.int32, (edge // 2, LANES), 1) < edge
    c = map_ref[0, : edge // 2]
    turned = pltpu.roll(c, edge, 1)
    rows = [jnp.where(left, c, 0.0), jnp.where(left, turned, 0.0)]
    rows += [jnp.where(left, 0.0, turned), jnp.where(left, 0.0, c)]
    maps_hi, maps_lo = split(jnp.concatenate(rows, axis=0))
    maps = jnp.concatenate([maps_hi, maps_lo], axis=1)
    for swapped, (high_ref, low_ref) in enumerate(((hi_ref, lo_ref), (hi_swapped_ref, lo_swapped_ref))):
        both = lax.dot_general(high_ref[...], ray_both, NT, preferred_element_type=jnp.float32)
        first = both[:, :LANES] + (
            both[:, LANES:] + lax.dot_general(low_ref[...], ray_hi, NT, preferred_element_type=jnp.float32)
        )
        first_hi, first_lo = split(first)
        for couple in range(planes // 2):
            at = [slice((2 * couple + i) * lateral, (2 * couple + i + 1) * lateral) for i in range(2)]
            high = jnp.concatenate([first_hi[i] for i in at], axis=1)
            low = jnp.concatenate([first_lo[i] for i in at], axis=1)
            second = lax.dot_general(
                maps, jnp.concatenate([high, high], axis=0), NN, preferred_element_type=jnp.float32
            ) + lax.dot_general(maps_hi, low, NN, preferred_element_type=jnp.float32)
            for i in range(2):
                plane = swapped * planes + 2 * couple + i
                for d in range(depth):
                    base = d * per
                    a = second[base : base + SUB, i * LANES : (i + 1) * LANES]
                    b = second[base + SUB : base + 2 * SUB, i * LANES : (i + 1) * LANES]
                    out_ref[pl.ds(starts[d] + plane * SUB, SUB), :] = jnp.where(half, a, b)
    for d in range(depth):
        u = d * per // edge
        out_ref[pl.ds(starts[d] + block_rows - 1, 1), :] = coef_ref[u : u + 1]


def render_kernel(step_length, planes, order, turn, recv_ref, maps_hi_ref, maps_lo_ref, entry_ref, out_ref):
    block_rows = planes * SUB + 1
    sources = len(order)
    columns, rows = entry_ref.shape
    bricks = steps = SUB
    maps_hi = maps_hi_ref[...]
    maps = jnp.concatenate([maps_hi, maps_hi], axis=0)
    maps_lo = maps_lo_ref[...]

    ends = [(order.index((0, b)) + 1) * block_rows for b in range(bricks)]
    packed = jnp.concatenate([recv_ref[end - 1 : end] for end in ends], axis=0)
    lane = lax.broadcasted_iota(jnp.int32, (bricks, rows), 1)
    upper = lane >= rows // 2
    coef = []
    for ch in range(COEF):
        low = jnp.broadcast_to(packed[:, ch : ch + 1], (bricks, rows))
        high = jnp.broadcast_to(packed[:, COEF + ch : COEF + ch + 1], (bricks, rows))
        coef.append(jnp.where(upper, high, low))
    brick = lax.broadcasted_iota(jnp.int32, (bricks, rows), 0)

    shown = [[None] * columns for _ in range(3)]
    for x in range(SUB):
        cells = jnp.concatenate(
            [recv_ref[pl.ds(p * SUB + x, sources, stride=block_rows), :] for p in range(planes)], axis=0
        )
        high, low = split(cells.T)
        samples = lax.dot_general(
            jnp.concatenate([high, low], axis=1), maps, NN, preferred_element_type=jnp.float32
        ) + lax.dot_general(high, maps_lo, NN, preferred_element_type=jnp.float32)
        for m in range(2):
            c = m * SUB + x
            live = jnp.where(entry_ref[c : c + 1, :] <= brick, -step_length * LOG2E, 0.0)
            total = jnp.zeros((bricks, rows), jnp.float32)
            before = jnp.ones((bricks, rows), jnp.float32)
            colours = [jnp.zeros((bricks, rows), jnp.float32) for _ in range(3)]
            for s in range(steps):
                at = (m * steps + s) * bricks
                v = samples[at : at + bricks]
                total = total + live * softplus(coef[6] * v + coef[7])
                after = jnp.exp2(total)
                weight = before - after
                before = after
                for ch in range(3):
                    colours[ch] = colours[ch] + weight * softplus(coef[ch] * v + coef[3 + ch])
            front = jnp.where(brick >= 1, pltpu.roll(total, 1, 0), 0.0)
            for shift in (1, 2, 4):
                front = front + jnp.where(brick >= shift, pltpu.roll(front, shift, 0), 0.0)
            reach = jnp.exp2(front)
            for ch in range(3):
                shown[ch][c] = jnp.sum(reach * colours[ch], axis=0, keepdims=True)
    blank = jnp.zeros((LANES // 2 - 3 * columns, rows), jnp.float32)
    image = jnp.concatenate([r for ch in shown for r in ch] + [blank], axis=0)
    image = jnp.concatenate([image, image], axis=0).T
    left = lax.broadcasted_iota(jnp.int32, (SUB, LANES), 1) < LANES // 2
    for n, d in enumerate(turn):
        at = d * 2 * SUB
        out_ref[n] = jnp.where(left, image[at : at + SUB], image[at + SUB : at + 2 * SUB])


def unpack_kernel(columns, turn, recv_ref, out_ref):
    owner = lax.broadcasted_iota(jnp.int32, (SUB, LANES), 1) // columns
    for ch in range(3):
        for h in range(2):
            out = jnp.zeros((SUB, LANES), jnp.float32)
            for n, s in enumerate(turn):
                moved = pltpu.roll(recv_ref[n], ((s - ch) * columns - h * (LANES // 2)) % LANES, 1)
                out = jnp.where(owner == s, moved, out)
            out_ref[0, ch, h * SUB : (h + 1) * SUB] = out


def small():
    return pltpu.CompilerParams(vmem_limit_bytes=16 * 1024 * 1024)


def orders(views, depth):
    chips = views // CORES
    order = [(x, z * 2 + y) for y in range(2) for x in range(chips) for z in range(depth // 2)]
    first = order.index((chips - 1, depth // 2 + 1))
    turn = depth // 2 + 1
    return order[first:] + order[:first], list(range(turn, depth)) + list(range(turn))


def vmem():
    return pl.BlockSpec(memory_space=pltpu.VMEM)


def hbm():
    return pl.BlockSpec(memory_space=pltpu.HBM)


def in_hbm(x):
    return pltpu.with_memory_space_constraint(x, pltpu.HBM)


def smem():
    return pl.BlockSpec(memory_space=pltpu.SMEM)


def with_kernels(volume, step_weights, row_interp, col_interp, tf_table, materials, entry):
    views = lax.axis_size("view")
    steps, edge = step_weights.shape[1:]
    depth = lax.axis_size("depth")
    planes, lateral, span = volume.shape
    devices = views * depth
    per = lateral // depth
    rows = devices * planes
    step_length = 2.0 / (steps * depth)
    tiles_y = lateral // edge
    block_rows = CORES * planes * SUB + 1
    order, turn = orders(views, depth)
    groups = [[(x * CORES + core) * depth + d for x, d in order] for core in range(CORES)]
    depth_at = lax.axis_index("depth").reshape(1)
    view_at = lax.axis_index("view").reshape(1)
    slab = lax.ppermute(volume, "view", [(i, i ^ 1) for i in range(views)])
    own, row, entry_all, coef = pl.pallas_call(
        fetch_kernel,
        out_shape=[
            jax.ShapeDtypeStruct((1, edge // 2 + steps, 2 * edge), jnp.float32),
            jax.ShapeDtypeStruct(row_interp.shape, row_interp.dtype),
            jax.ShapeDtypeStruct(entry.shape, entry.dtype),
            jax.ShapeDtypeStruct((tiles_y, LANES), jnp.float32),
        ],
        in_specs=[hbm()] * 6,
        out_specs=[vmem()] * 4,
        scratch_shapes=[
            pltpu.VMEM(step_weights.shape, jnp.float32),
            pltpu.VMEM(col_interp.shape, jnp.float32),
            pltpu.SMEM((materials.shape[0], 1, tiles_y), jnp.int32),
            pltpu.SMEM(tf_table.shape, jnp.float32),
            pltpu.SemaphoreType.DMA((6,)),
        ],
        compiler_params=small(),
        cost_estimate=pl.CostEstimate(flops=4_000_000_000, bytes_accessed=8_000_000, transcendentals=0),
        name="fetch",
    )(*map(in_hbm, (step_weights, col_interp, materials.transpose(0, 2, 1), tf_table, row_interp, entry)))
    far = lax.ppermute(own, "view", [(i, i ^ CORES) for i in range(views)])
    hi, lo, maps_hi, maps_lo, entry_own = pl.pallas_call(
        functools.partial(prepare_kernel, order, planes),
        out_shape=[
            jax.ShapeDtypeStruct((planes * lateral, span), jnp.bfloat16),
            jax.ShapeDtypeStruct((planes * lateral, span), jnp.bfloat16),
            jax.ShapeDtypeStruct((rows, rows), jnp.bfloat16),
            jax.ShapeDtypeStruct((rows, rows), jnp.bfloat16),
            jax.ShapeDtypeStruct((per, rows), jnp.int32),
        ],
        in_specs=[smem()] * 2 + [vmem()] * 3,
        out_specs=[vmem()] * 5,
        scratch_shapes=[pltpu.VMEM((rows, rows), jnp.float32), pltpu.VMEM((rows, rows), jnp.float32)],
        compiler_params=small(),
        cost_estimate=pl.CostEstimate(flops=2_000_000_000, bytes_accessed=4_000_000, transcendentals=0),
        name="prepare",
    )(view_at, depth_at, volume, row, entry_all)
    sent = jax.ShapeDtypeStruct((len(order) * block_rows, LANES), jnp.float32)
    halves = jax.ShapeDtypeStruct((planes * lateral, span), jnp.bfloat16)
    blocks, *swapped = pl.pallas_call(
        functools.partial(send_kernel, order, depth, planes, 0),
        out_shape=[sent, halves, halves],
        in_specs=[smem()] + [vmem()] * 5,
        out_specs=[vmem()] * 3,
        compiler_params=small(),
        cost_estimate=pl.CostEstimate(flops=1_000_000_000, bytes_accessed=2_000_000, transcendentals=0),
        name="send_0",
    )(view_at, hi, lo, coef, own, slab)
    blocks = pl.pallas_call(
        functools.partial(send_kernel, order, depth, planes, 1),
        out_shape=sent,
        in_specs=[smem()] + [vmem()] * 7,
        out_specs=vmem(),
        input_output_aliases={7: 0},
        compiler_params=small(),
        cost_estimate=pl.CostEstimate(flops=1_000_000_000, bytes_accessed=2_000_000, transcendentals=0),
        name="send_1",
    )(view_at, hi, lo, coef, far, *swapped, blocks)
    blocks = blocks.reshape(len(order), block_rows, 1, LANES)
    recv = lax.all_to_all(blocks, ("view", "depth"), split_axis=0, concat_axis=0, tiled=True, axis_index_groups=groups)
    recv = recv.reshape(len(order) * block_rows, LANES)
    image = pl.pallas_call(
        functools.partial(render_kernel, step_length, CORES * planes, order, turn),
        out_shape=jax.ShapeDtypeStruct((depth, SUB, LANES), jnp.float32),
        in_specs=[vmem()] * 4,
        out_specs=vmem(),
        compiler_params=small(),
        name="render",
    )(recv, maps_hi, maps_lo, entry_own)
    turned = lax.all_to_all(image, "depth", split_axis=0, concat_axis=0, tiled=True, axis_index_groups=[turn])
    return pl.pallas_call(
        functools.partial(unpack_kernel, per, turn),
        out_shape=jax.ShapeDtypeStruct((1, 3, rows // depth, lateral), jnp.float32),
        in_specs=[vmem()],
        out_specs=vmem(),
        compiler_params=small(),
        name="unpack",
    )(turned)


def with_arrays(volume, step_weights, row_interp, col_interp, tf_table, materials, entry):
    all_steps = lax.all_gather(step_weights, "view", axis=0, tiled=True)
    all_cols = lax.all_gather(col_interp, "view", axis=0, tiled=True)
    views, steps, edge = all_steps.shape
    depth = lax.axis_size("depth")
    planes, lateral, _ = volume.shape
    devices = views * depth
    per = lateral // depth
    rows = devices * planes
    tiles_z, tiles_y = materials.shape[:2]
    step_length = 2.0 / (steps * depth)
    cells = volume.reshape(planes, tiles_y, edge, depth, edge)
    first = jnp.einsum("pujbi,vsi->vpujbs", cells, all_steps, precision=HIGHEST)
    second = jnp.einsum("vpujbs,vcj->vpucbs", first, all_cols, precision=HIGHEST)
    second = second.reshape(views, planes, depth, per, depth, steps).transpose(0, 2, 1, 3, 4, 5)
    second = second.reshape(devices, planes * per * depth * steps)
    own = tf_table[materials[:, :, 0]].transpose(1, 0, 2).reshape(tiles_y, tiles_z * COEF)
    own = jnp.tile(jnp.repeat(own, edge // per, axis=0), (views, 1))
    payload = jnp.concatenate([second, own], axis=1)
    payload = jnp.pad(payload, ((0, 0), (0, -payload.shape[1] % LANES)))
    payload = payload.reshape(devices, -1, 1, LANES)
    recv = lax.all_to_all(payload, ("view", "depth"), split_axis=0, concat_axis=0, tiled=True)
    recv = recv.reshape(devices, -1)
    size = second.shape[1]
    coef = recv[:depth, size : size + tiles_z * COEF].reshape(depth, tiles_z, COEF)
    coef = jnp.repeat(coef.transpose(2, 1, 0), edge, axis=1)[:, :, None, :, None]
    third = recv[:, :size].reshape(tiles_z, edge, per, depth, steps)
    third = jnp.einsum("tkcbs,rk->trcbs", third, row_interp[0], precision=HIGHEST)
    samples = third.reshape(rows, per, depth, steps)
    entry_own = lax.dynamic_slice_in_dim(entry[0], lax.axis_index("depth") * per, per, 1)
    live = (entry_own[:, :, None] <= jnp.arange(depth)).astype(jnp.float32)
    tau = step_length * live[..., None] * jax.nn.softplus(coef[6] * samples + coef[7])
    flat = tau.reshape(rows, per, depth * steps)
    earlier = (jnp.cumsum(flat, axis=2) - flat).reshape(tau.shape)
    weights = jnp.exp(-earlier) * (1.0 - jnp.exp(-tau))
    emission = jax.nn.softplus(coef[0:3] * samples + coef[3:6])
    image = jnp.sum(weights * emission, axis=(3, 4))
    turned = lax.all_to_all(image, "depth", split_axis=1, concat_axis=2, tiled=True)
    return turned[None]


def shards(volume, step_weights, row_interp, col_interp, tf_table, materials, entry):
    views = lax.axis_size("view")
    depth = lax.axis_size("depth")
    planes, lateral, span = volume.shape
    steps, edge = step_weights.shape[1:]
    rows = views * depth * planes
    fits = (
        depth == SUB
        and steps == SUB
        and edge == LANES // 2
        and lateral == LANES
        and rows == LANES
        and views == 2 * CORES
        and span == depth * edge
    )
    run = with_kernels if fits else with_arrays
    return run(volume, step_weights, row_interp, col_interp, tf_table, materials, entry)


def solution(mesh):
    placed = (
        P(("view", "depth"), None, None),
        P("view", None, None),
        P("view", None, None),
        P("view", None, None),
        P(),
        P(None, None, "depth"),
        P("view", None, None),
    )
    return jax.shard_map(
        shards,
        mesh=mesh,
        in_specs=placed,
        out_specs=P("view", None, "depth", None),
        check_vma=False,
    )
```
